32 devices in a mesh: param: 16 (over z, x, core), qoi: 2 (over y).
Axes of the slice: x: 2, y: 2, z: 4, core: 2. Of those that a mesh axis runs over, the one named last changes fastest.
Arguments:
- samples: bfloat16 [16, 5120, 420], P('qoi', 'param'), may hold values from -6 to 6
- operator_rows: bfloat16 [8, 5120, 2, 512], P(None, 'param', None, 'qoi'), may hold values from -0.0625 to 0.0625
- block_start: int32 [1], replicated, may hold values from 0 to 203
- gauge_group: int32 [512], P('qoi'), may hold values from 0 to 15
Outputs:
- qoi_spectrum: float32 [16, 2, 8, 512], P('param', None, None, 'qoi')
- segment_response: float32 [16, 2, 8, 16], P('param')
The draws below stay inside these ranges and needn't reach their ends.
Inputs may be any that keep to these rules, and one draw needn't show every extreme that they name: `block_start`: the block's frequencies lie among the 211 frequencies of a real transform.
All inputs are finite; a program needn't handle non-finite values.
Results may differ from the reference program's by a relative error of at most 0.005.
Values may be sent and summed in bfloat16 or wider, within the bound.
A program may use at most 64 MiB of HBM per device.

```python
import math
import jax
import jax.numpy as jnp
from jax import lax

NF = 8
NT = 420
GROUPS = 16
SAMPLES = 16
NP = 5120
GAUGES = 512


def place_ends(result, rng, least, largest):
    longest = result.shape.index(max(result.shape))
    spots = []
    for shift in (0, 1):
        where = [jax.random.randint(jax.random.fold_in(rng, axis), (), 0, length) for axis, length in enumerate(result.shape)]
        where[longest] = (where[longest] + shift) % result.shape[longest]
        spots.append(tuple(where))
    return result.at[spots[0]].set(least).at[spots[1]].set(largest)


def raised(result, own_key, source, target, shards_of, factor):
    owner, partner = [(jnp.arange(result.shape[dim]) // (result.shape[dim] // shards_of)).reshape([-1 if axis == dim else 1 for axis in range(result.ndim)]) for dim in (source, target)]
    chosen = jax.random.permutation(own_key, shards_of)[partner]
    strong = (owner == chosen) | (owner == (partner + shards_of // 2) % shards_of)
    return jnp.where(strong, factor * result, result)


def block_scale(own_key, extent, split, least, largest):
    def one(dim, shards_of):
        steps = jax.random.uniform(jax.random.fold_in(jax.random.fold_in(own_key, 6), dim), (shards_of,), jnp.float32, least / len(split), largest / len(split))
        return jnp.repeat(jnp.exp(steps), extent[dim] // shards_of).reshape((-1,) + (1,) * (len(extent) - dim - 1))

    loudness = one(*split[0])
    for cut in split[1:]:
        loudness = loudness * one(*cut)
    return loudness


def noise(rng, shape, width, most, shards=(), held_as=jnp.bfloat16):
    loudness = block_scale(rng, shape, shards, -0.22, 0.18) if shards else 1.0
    drawn = jax.random.normal(rng, shape, jnp.float32) * width * loudness
    return jnp.minimum(jnp.maximum(drawn, -most), most).astype(held_as)


def gaussian_with(key, dims, scale, reach, split, heavy, kind=jnp.bfloat16):
    array = scale * jax.random.normal(key, dims, jnp.float32)
    if split:
        array = array * block_scale(key, dims, split, -0.22, 0.18)
    return jnp.clip(raised(array, jax.random.fold_in(key, 3), *heavy), -reach, reach).astype(kind)


def setup_inputs(seed: int = 0) -> dict:
    key_of = jax.random.split(jax.random.key(seed), 5)
    return {
        "samples": gaussian_with(key_of[0], (SAMPLES, NP, NT), 1.0, 6.0, ((0, 2), (1, 16)), (1, 0, 16, 2.0)),
        "operator_rows": noise(key_of[1], (NF, NP, 2, GAUGES), (2 * NP) ** -0.5, 0.0625, ((1, 16), (3, 2))),
        "block_start": jax.random.randint(key_of[2], (1,), 0, NT // 2 + 2 - NF).astype(jnp.int32),
        "gauge_group": place_ends(jax.random.randint(key_of[3], (GAUGES,), 0, GROUPS), jax.random.fold_in(key_of[3], 1), 0, GROUPS - 1).astype(jnp.int32),
    }


def sample_spectrum(series, first):
    spectrum_all = jnp.fft.rfft(series.astype(jnp.float32), axis=-1)
    window = lax.dynamic_slice_in_dim(spectrum_all, first, NF, 1)
    factor = 1.0 / math.sqrt(NT)
    real_part = (jnp.real(window) * factor).astype(jnp.bfloat16)
    imag_part = (jnp.imag(window) * factor).astype(jnp.bfloat16)
    return jnp.stack([real_part, imag_part], axis=0)

def frequency_response(paired):
    spectrum_f, weights_f = paired
    real_w = weights_f[:, 0, :]
    imag_w = weights_f[:, 1, :]
    real_real = jnp.dot(spectrum_f[0], real_w, preferred_element_type=jnp.float32)
    imag_imag = jnp.dot(spectrum_f[1], imag_w, preferred_element_type=jnp.float32)
    real_imag = jnp.dot(spectrum_f[0], imag_w, preferred_element_type=jnp.float32)
    imag_real = jnp.dot(spectrum_f[1], real_w, preferred_element_type=jnp.float32)
    return jnp.stack([real_real - imag_imag, real_imag + imag_real], axis=0)

def reference(samples, operator_rows, block_start, gauge_group):
    first = block_start[0].astype(jnp.int32)
    spectra = lax.map(lambda series: sample_spectrum(series, first), samples)
    spectra = jnp.transpose(spectra, (3, 1, 0, 2))
    responses = lax.map(frequency_response, (spectra, operator_rows))
    qoi_spectrum = jnp.transpose(responses, (2, 1, 0, 3))
    onehot = (gauge_group[:, None] == jnp.arange(GROUPS, dtype=jnp.int32)[None, :]).astype(jnp.float32)
    segment = jnp.dot(qoi_spectrum.reshape(-1, GAUGES), onehot, precision=lax.Precision.HIGHEST, preferred_element_type=jnp.float32)
    segment_response = segment.reshape(SAMPLES, 2, NF, GROUPS) * math.sqrt(GROUPS / GAUGES)
    return (qoi_spectrum, segment_response)
```

```python
import functools
import math

import jax
import jax.numpy as jnp
from jax import lax
from jax.experimental import pallas as pl
from jax.experimental.pallas import tpu as pltpu
from jax.sharding import PartitionSpec as P

GROUPS = 16
LANES = 128
PARTS = 4
LOADS = 4
MESH = pl.DeviceIdType.MESH
NT_DIMS = (((1,), (1,)), ((), ()))


def build_table(start, freq_count, steps_count, repeat, table):
    shape = (freq_count, steps_count * repeat)
    steps = lax.broadcasted_iota(jnp.int32, shape, 1) // repeat
    freqs = lax.broadcasted_iota(jnp.int32, shape, 0) + start
    turns = (steps * freqs).astype(jnp.float32)
    whole = jnp.floor((turns + 0.5) * (1.0 / steps_count))
    phases = (turns - whole * steps_count) * (2.0 * math.pi / steps_count)
    scale = 1.0 / math.sqrt(steps_count)
    waves = [jnp.cos(phases) * scale, jnp.sin(phases) * -scale]
    highs = [wave.astype(jnp.bfloat16).astype(jnp.float32) for wave in waves]
    lows = [wave - high for wave, high in zip(waves, highs)]
    full = (repeat, steps_count * repeat)
    keep = lax.broadcasted_iota(jnp.int32, full, 1) % repeat == lax.broadcasted_iota(
        jnp.int32, full, 0
    )
    for level, pair in enumerate((highs, lows)):
        for f in range(freq_count):
            rows = jnp.concatenate(
                [jnp.where(keep, jnp.broadcast_to(wave[f : f + 1], full), 0.0) for wave in pair],
                axis=0,
            )
            first = (level * freq_count + f) * 2 * repeat
            table[pl.ds(first, 2 * repeat), :] = rows.astype(jnp.bfloat16)


def kernel(
    param_count, qoi_count, start_ref, group_hbm, samples_hbm, rows_hbm,
    out_ref, seg_ref,
    group_ref, samples, table, weights, loose, dense, dense_tail, hot, line, line_tail, product, outgoing, incoming, joined, shares, gathered,
    group_sem, samples_sem, weights_sem, line_send, line_recv, out_send, out_recv, share_send, share_recv,
):
    steps_count, sample_local, param_local = samples.shape
    freq_count = weights.shape[0]
    gauge_local = group_ref.shape[1]
    halves = gauge_local // LANES
    sample_total = sample_local * qoi_count
    aligned = param_local // LANES * LANES
    tail = param_local - aligned
    pair_rows = 2 * sample_local
    half_freqs = freq_count // 2
    me_p = lax.axis_index("param")
    me_q = lax.axis_index("qoi")

    edges = [steps_count * part // PARTS // 32 * 32 for part in range(PARTS)] + [steps_count]
    spans = [pl.ds(edges[part], edges[part + 1] - edges[part]) for part in range(PARTS)]
    sample_copies = [
        pltpu.make_async_copy(samples_hbm.at[span], samples.at[span], samples_sem.at[part])
        for part, span in enumerate(spans)
    ]
    for copy in sample_copies:
        copy.start()
    group_copy = pltpu.make_async_copy(group_hbm, group_ref, group_sem)
    group_copy.start()
    per_load = freq_count // LOADS
    loads = [pl.ds(load * per_load, per_load) for load in range(LOADS)]
    weight_copies = [
        pltpu.make_async_copy(rows_hbm.at[load], weights.at[load], weights_sem.at[index])
        for index, load in enumerate(loads)
    ]

    barrier = pltpu.get_barrier_semaphore()
    for far in range(qoi_count):
        for offset in range(param_count):
            if far or offset:
                pl.semaphore_signal(
                    barrier,
                    inc=1,
                    device_id=(
                        lax.rem(me_p + offset, param_count), lax.rem(me_q + far, qoi_count)
                    ),
                    device_id_type=MESH,
                )

    build_table(start_ref[0], freq_count, steps_count, sample_local, table)

    main = ends = None
    for part in range(PARTS):
        first, count = edges[part], edges[part + 1] - edges[part]
        sample_copies[part].wait()
        if part == PARTS // 2:
            for copy in weight_copies:
                copy.start()
        block = samples[spans[part]].reshape(count * sample_local, param_local)
        turn = table[:, first * sample_local : (first + count) * sample_local]
        term = jnp.dot(turn, block[:, :aligned], preferred_element_type=jnp.float32)
        last = jnp.dot(turn, block[:, aligned:], preferred_element_type=jnp.float32)
        main = term if main is None else main + term
        ends = last if ends is None else ends + last
    half = 2 * freq_count * sample_local
    spectrum = (main[:half] + main[half:]).astype(jnp.bfloat16)
    for chunk in range(aligned // LANES):
        line[chunk, me_q] = spectrum[:, chunk * LANES : (chunk + 1) * LANES].reshape(
            freq_count, pair_rows, LANES
        )
    spectrum = ends[:half] + ends[half:]
    line_tail[me_q] = (
        jnp.concatenate([spectrum[: half // 2], spectrum[half // 2 :]], axis=1)
        .astype(jnp.bfloat16)
        .reshape(half_freqs, pair_rows, 2 * tail)
    )

    pl.semaphore_wait(barrier, qoi_count * param_count - 1)
    buffers = [line.at[chunk] for chunk in range(aligned // LANES)] + [line_tail]
    line_waits = []
    for index, buffer in enumerate(buffers):
        for offset in range(1, qoi_count):
            pltpu.make_async_remote_copy(
                src_ref=buffer.at[me_q],
                dst_ref=buffer.at[me_q],
                send_sem=line_send.at[index],
                recv_sem=line_recv.at[index],
                device_id=(me_p, lax.rem(me_q + offset, qoi_count)),
                device_id_type=MESH,
            ).start()
        others = buffer.at[pl.ds(0, qoi_count - 1)]
        line_waits.append(
            pltpu.make_async_remote_copy(
                src_ref=others,
                dst_ref=others,
                send_sem=line_send.at[index],
                recv_sem=line_recv.at[index],
                device_id=(me_p, lax.rem(me_q + 1, qoi_count)),
                device_id_type=MESH,
            )
        )

    for f in range(freq_count):
        if f % per_load == 0:
            weight_copies[f // per_load].wait()
        loose[...] = weights[f].astype(jnp.float32)
        for j in range(halves):
            columns = pl.ds(j * LANES, LANES)
            for part in range(2):
                piece = loose[
                    pl.ds(2 * j + part, param_local, stride=2 * halves), :
                ].astype(jnp.bfloat16)
                dense[f, part, :, columns] = piece[:aligned]
                dense_tail[f % half_freqs, part, pl.ds(f // half_freqs * tail, tail), columns] = (
                    piece[aligned:]
                )

    group_copy.wait()
    slots = lax.broadcasted_iota(jnp.int32, (LANES, gauge_local), 0)
    for f in range(freq_count):
        place = (freq_count - f) % freq_count * GROUPS
        hot[f] = (slots == group_ref[...] + place).astype(jnp.float32).astype(jnp.bfloat16)

    def combine(real_side, imag_side):
        reals, imags = [], []
        for q in range(qoi_count):
            low, mid, high = q * pair_rows, q * pair_rows + sample_local, (q + 1) * pair_rows
            reals.append(real_side[low:mid] - imag_side[mid:high])
            imags.append(imag_side[low:mid] + real_side[mid:high])
        return [jnp.concatenate(reals, axis=0), jnp.concatenate(imags, axis=0)]

    def place_of(k, f):
        return pl.ds((k * freq_count + f) * sample_total, sample_total)

    for chunk in range(aligned // LANES):
        line_waits[chunk].wait_recv()
        for f in range(freq_count):
            left = jnp.concatenate([line[chunk, q, f] for q in range(qoi_count)], axis=0)
            sides = [
                jnp.dot(
                    left,
                    dense[f, part, chunk * LANES : (chunk + 1) * LANES, :],
                    preferred_element_type=jnp.float32,
                )
                for part in range(2)
            ]
            for k, value in enumerate(combine(*sides)):
                for j in range(halves):
                    here = value[:, j * LANES : (j + 1) * LANES]
                    if chunk:
                        here = here + product[j, place_of(k, f), :]
                    product[j, place_of(k, f), :] = here

    line_waits[-1].wait_recv()
    lane = lax.broadcasted_iota(jnp.int32, (qoi_count * pair_rows, 2 * tail), 1)
    segment = None
    for f in range(freq_count):
        left = jnp.concatenate(
            [line_tail[q, f % half_freqs] for q in range(qoi_count)], axis=0
        )
        left = jnp.where((lane >= tail) == (f >= half_freqs), left.astype(jnp.float32), 0.0)
        left = left.astype(jnp.bfloat16)
        sides = [
            jnp.dot(left, dense_tail[f % half_freqs, part], preferred_element_type=jnp.float32)
            for part in range(2)
        ]
        finals = []
        for k, value in enumerate(combine(*sides)):
            wide = []
            for j in range(halves):
                here = value[:, j * LANES : (j + 1) * LANES] + product[j, place_of(k, f), :]
                product[j, place_of(k, f), :] = here
                wide.append(here)
            finals.append(jnp.concatenate(wide, axis=1))
        sums = lax.dot_general(
            jnp.concatenate(finals, axis=0).astype(jnp.bfloat16),
            hot[f],
            NT_DIMS,
            preferred_element_type=jnp.float32,
        )
        segment = sums if segment is None else segment + sums
    stripe = 2 * freq_count
    for r in range(sample_total):
        for j in range(halves):
            outgoing[r, :, j * LANES : (j + 1) * LANES] = product[
                j, pl.ds(r, stripe, stride=sample_total), :
            ].astype(jnp.bfloat16)
    for offset in range(1, param_count):
        target = lax.rem(me_p + offset, param_count)
        pltpu.make_async_remote_copy(
            src_ref=outgoing.at[target],
            dst_ref=incoming.at[me_p],
            send_sem=out_send,
            recv_sem=out_recv,
            device_id=(target, me_q),
            device_id_type=MESH,
        ).start()
    joined[...] = segment * math.sqrt(GROUPS / (gauge_local * qoi_count))
    for k in range(sample_total):
        shares[k] = joined[pl.ds(k, 2, stride=sample_total), :]
    mine = me_q * param_count + me_p
    for far in reversed(range(qoi_count)):
        for offset in range(param_count):
            if far or offset:
                target = lax.rem(me_p + offset, param_count)
                pltpu.make_async_remote_copy(
                    src_ref=shares.at[target],
                    dst_ref=gathered.at[mine],
                    send_sem=share_send,
                    recv_sem=share_recv,
                    device_id=(target, lax.rem(me_q + far, qoi_count)),
                    device_id_type=MESH,
                ).start()
    incoming[me_p] = outgoing[me_p]
    gathered[mine] = shares[me_p]

    aside = (lax.rem(me_p + 1, param_count), me_q)
    others = incoming.at[pl.ds(0, param_count - 1)]
    out_wait = pltpu.make_async_remote_copy(
        src_ref=others, dst_ref=others, send_sem=out_send, recv_sem=out_recv,
        device_id=aside, device_id_type=MESH,
    )
    others = gathered.at[pl.ds(0, qoi_count * param_count - 1)]
    share_wait = pltpu.make_async_remote_copy(
        src_ref=others, dst_ref=others, send_sem=share_send, recv_sem=share_recv,
        device_id=aside, device_id_type=MESH,
    )
    out_wait.wait_recv()
    total = incoming[0].astype(jnp.float32)
    for p in range(1, param_count):
        total = total + incoming[p].astype(jnp.float32)
    out_ref[...] = total.reshape(out_ref.shape)
    share_wait.wait_recv()
    final = gathered[0]
    for p in range(1, param_count * qoi_count):
        final = final + gathered[p]
    for k in range(2):
        rows = jnp.broadcast_to(final[k : k + 1], (freq_count, LANES))
        turned = pltpu.roll(rows, 0, 1, stride=GROUPS, stride_axis=0)
        seg_ref[0, k] = turned[:, :GROUPS]
    for wait in line_waits:
        wait.wait_send()
    out_wait.wait_send()
    share_wait.wait_send()


def writer(spectrum_ref, response_ref, spectrum_hbm, response_hbm, sems):
    copies = [
        pltpu.make_async_copy(spectrum_ref, spectrum_hbm, sems.at[0]),
        pltpu.make_async_copy(response_ref, response_hbm, sems.at[1]),
    ]
    for copy in copies:
        copy.start()
    for copy in copies:
        copy.wait()


def local(samples, operator_rows, block_start, gauge_group):
    sample_local, param_local, steps_count = samples.shape
    freq_count, _, _, gauge_local = operator_rows.shape
    param_count, qoi_count = lax.axis_size("param"), lax.axis_size("qoi")
    sample_total = sample_local * qoi_count
    halves = gauge_local // LANES
    depth = 2 * param_local
    stripe = 2 * freq_count
    aligned = param_local // LANES * LANES
    tail = param_local - aligned
    assert sample_total == param_count and freq_count * GROUPS == LANES
    assert 2 * tail == LANES and freq_count % LOADS == 0
    rows = operator_rows.reshape(freq_count, param_local, 2, halves, LANES)
    rows = rows.transpose(0, 1, 3, 2, 4).reshape(freq_count, depth * halves, LANES)
    dma = pltpu.SemaphoreType.DMA
    vmem = pl.BlockSpec(memory_space=pltpu.VMEM)
    hbm = pl.BlockSpec(memory_space=pltpu.HBM)
    shapes = (
        jax.ShapeDtypeStruct((1, 2, freq_count, gauge_local), jnp.float32),
        jax.ShapeDtypeStruct((1, 2, freq_count, GROUPS), jnp.float32),
    )
    found = pl.pallas_call(
        functools.partial(kernel, param_count, qoi_count),
        out_shape=shapes,
        in_specs=[pl.BlockSpec(memory_space=pltpu.SMEM), hbm, hbm, hbm],
        out_specs=(vmem, vmem),
        scratch_shapes=[
            pltpu.VMEM((1, gauge_local), jnp.int32),
            pltpu.VMEM((steps_count, sample_local, param_local), jnp.bfloat16),
            pltpu.VMEM((4 * freq_count * sample_local, steps_count * sample_local), jnp.bfloat16),
            pltpu.VMEM((freq_count, depth * halves, LANES), jnp.bfloat16),
            pltpu.VMEM((depth * halves, LANES), jnp.float32),
            pltpu.VMEM((freq_count, 2, aligned, gauge_local), jnp.bfloat16),
            pltpu.VMEM((freq_count // 2, 2, 2 * tail, gauge_local), jnp.bfloat16),
            pltpu.VMEM((freq_count, LANES, gauge_local), jnp.bfloat16),
            pltpu.VMEM((aligned // LANES, qoi_count, freq_count, 2 * sample_local, LANES), jnp.bfloat16),
            pltpu.VMEM((qoi_count, freq_count // 2, 2 * sample_local, 2 * tail), jnp.bfloat16),
            pltpu.VMEM((halves, stripe * sample_total, LANES), jnp.float32),
            pltpu.VMEM((sample_total, stripe, gauge_local), jnp.bfloat16),
            pltpu.VMEM((param_count, stripe, gauge_local), jnp.bfloat16),
            pltpu.VMEM((2 * sample_total, LANES), jnp.float32),
            pltpu.VMEM((sample_total, 2, LANES), jnp.float32),
            pltpu.VMEM((qoi_count * param_count, 2, LANES), jnp.float32),
            dma(()),
            dma((PARTS,)),
            dma((LOADS,)),
            dma((aligned // LANES + 1,)),
            dma((aligned // LANES + 1,)),
            dma(()),
            dma(()),
            dma(()),
            dma(()),
        ],
        compiler_params=pltpu.CompilerParams(
            collective_id=0, has_side_effects=True, vmem_limit_bytes=53 * 2**20
        ),
    )(
        block_start,
        pltpu.with_memory_space_constraint(gauge_group.reshape(1, gauge_local), pltpu.HBM),
        samples.transpose(2, 0, 1),
        rows,
    )
    return pl.pallas_call(
        writer,
        out_shape=shapes,
        in_specs=[vmem, vmem],
        out_specs=(pl.BlockSpec(memory_space=pl.ANY), pl.BlockSpec(memory_space=pl.ANY)),
        scratch_shapes=[dma((2,))],
    )(*[pltpu.with_memory_space_constraint(array, pltpu.VMEM) for array in found])


def solution(mesh):
    return jax.shard_map(
        local,
        mesh=mesh,
        in_specs=(P("qoi", "param", None), P(None, "param", None, "qoi"), P(), P("qoi")),
        out_specs=(P("param", None, None, "qoi"), P("param", None, None, None)),
        check_vma=False,
    )
```

```python
import functools
import math

import jax
import jax.numpy as jnp
from jax import lax
from jax.experimental import pallas as pl
from jax.experimental.pallas import tpu as pltpu
from jax.sharding import PartitionSpec as P

GROUPS = 16
LANES = 128
LOADS = 4
MESH = pl.DeviceIdType.MESH
NT_DIMS = (((1,), (1,)), ((), ()))


def build_table(start, freq_count, steps_count, count, repeat, table):
    shape = (freq_count, count * repeat)
    steps = lax.broadcasted_iota(jnp.int32, shape, 1) // repeat
    freqs = lax.broadcasted_iota(jnp.int32, shape, 0) + start
    turns = (steps * freqs).astype(jnp.float32)
    whole = jnp.floor((turns + 0.5) * (1.0 / steps_count))
    phases = (turns - whole * steps_count) * (2.0 * math.pi / steps_count)
    scale = 1.0 / math.sqrt(steps_count)
    waves = [jnp.cos(phases) * scale, jnp.sin(phases) * -scale]
    highs = [wave.astype(jnp.bfloat16).astype(jnp.float32) for wave in waves]
    lows = [wave - high for wave, high in zip(waves, highs)]
    full = (repeat, count * repeat)
    keep = lax.broadcasted_iota(jnp.int32, full, 1) % repeat == lax.broadcasted_iota(
        jnp.int32, full, 0
    )
    for level, pair in enumerate((highs, lows)):
        for f in range(freq_count):
            rows = jnp.concatenate(
                [jnp.where(keep, jnp.broadcast_to(wave[f : f + 1], full), 0.0) for wave in pair],
                axis=0,
            )
            first = (level * freq_count + f) * 2 * repeat
            table[pl.ds(first, 2 * repeat), :] = rows.astype(jnp.bfloat16)


def kernel(
    param_count, qoi_count, start_ref, group_hbm, samples_hbm, rows_hbm,
    out_ref, seg_ref,
    group_ref, samples, table, weights, loose, dense, dense_tail, hot, line, line_tail, near, far, outgoing, incoming, joined, shares, gathered,
    group_sem, samples_sem, weights_sem, line_send, line_recv, out_send, out_recv, share_send, share_recv, known,
):
    steps_count, sample_local, param_local = samples.shape
    freq_count = weights.shape[0]
    gauge_local = group_ref.shape[1]
    halves = gauge_local // LANES
    aligned = param_local // LANES * LANES
    tail = param_local - aligned
    chunks = aligned // LANES
    pair_rows = 2 * sample_local
    half_freqs = freq_count // 2
    half_steps = steps_count // 2
    stripe = 2 * freq_count
    inner = 2 ** (int(math.log2(param_count)) // 2)
    me_p = lax.axis_index("param")
    me_q = lax.axis_index("qoi")
    base = me_p // inner * inner

    contacts = []
    for turn in range(1, param_count // inner):
        contacts.append((lax.rem(me_p + turn * inner, param_count), me_q))
    for other in reversed(range(qoi_count)):
        for turn in range(inner):
            if other or turn:
                contacts.append(
                    (base + lax.rem(me_p + turn, inner), lax.rem(me_q + other, qoi_count))
                )
    barrier = pltpu.get_barrier_semaphore()
    spans = [pl.ds(0, half_steps), pl.ds(half_steps, half_steps)]
    sample_copies = [
        pltpu.make_async_copy(samples_hbm.at[span], samples.at[span], samples_sem.at[part])
        for part, span in enumerate(spans)
    ]
    for copy in sample_copies:
        copy.start()
    for contact in contacts:
        pl.semaphore_signal(barrier, inc=1, device_id=contact, device_id_type=MESH)
    group_copy = pltpu.make_async_copy(group_hbm, group_ref, group_sem)
    group_copy.start()
    per_load = freq_count // LOADS
    loads = [pl.ds(load * per_load, per_load) for load in range(LOADS)]
    weight_copies = [
        pltpu.make_async_copy(rows_hbm.at[load], weights.at[load], weights_sem.at[index])
        for index, load in enumerate(loads)
    ]

    start = start_ref[0]
    build_table(start, freq_count, steps_count, half_steps, sample_local, table)

    turns = table[...]
    blocks, sides = [], []
    half = freq_count * pair_rows
    for part in range(2):
        sample_copies[part].wait()
        if part == 0:
            for copy in weight_copies:
                copy.start()
        block = samples[spans[part]].reshape(half_steps * sample_local, param_local)
        both = jnp.dot(turns, block[:, :aligned], preferred_element_type=jnp.float32)
        sides.append(both[:half] + both[half:])
        blocks.append(block[:, aligned:])
    odd = lax.rem(start + lax.broadcasted_iota(jnp.int32, (half, LANES), 0) // pair_rows, 2)
    sign = 1.0 - 2.0 * odd.astype(jnp.float32)
    for chunk in range(chunks):
        columns = slice(chunk * LANES, (chunk + 1) * LANES)
        spectrum = sides[0][:, columns] + sign * sides[1][:, columns]
        line[chunk, me_q] = spectrum.astype(jnp.bfloat16).reshape(freq_count, pair_rows, LANES)
    both = jnp.dot(turns, jnp.concatenate(blocks, axis=1), preferred_element_type=jnp.float32)
    both = both[:half] + both[half:]
    both = both + sign * pltpu.roll(both, tail, 1)
    middle = half // 2
    lane = lax.broadcasted_iota(jnp.int32, (middle, LANES), 1)
    packed = jnp.where(lane < tail, both[:middle], both[middle:] * sign[middle:])
    line_tail[me_q] = packed.astype(jnp.bfloat16).reshape(half_freqs, pair_rows, LANES)

    pl.semaphore_wait(barrier, len(contacts))
    buffers = [line.at[chunk] for chunk in range(chunks)] + [line_tail]
    line_waits = []
    for index, buffer in enumerate(buffers):
        for offset in range(1, qoi_count):
            pltpu.make_async_remote_copy(
                src_ref=buffer.at[me_q],
                dst_ref=buffer.at[me_q],
                send_sem=line_send.at[index],
                recv_sem=line_recv.at[index],
                device_id=(me_p, lax.rem(me_q + offset, qoi_count)),
                device_id_type=MESH,
            ).start()
        others = buffer.at[pl.ds(0, qoi_count - 1)]
        line_waits.append(
            pltpu.make_async_remote_copy(
                src_ref=others,
                dst_ref=others,
                send_sem=line_send.at[index],
                recv_sem=line_recv.at[index],
                device_id=(me_p, lax.rem(me_q + 1, qoi_count)),
                device_id_type=MESH,
            )
        )
    for contact in contacts:
        pl.semaphore_signal(known, inc=1, device_id=contact, device_id_type=MESH)

    group_copy.wait()
    slots = lax.broadcasted_iota(jnp.int32, (LANES, gauge_local), 0)
    for f in range(freq_count):
        place = (freq_count - f) % freq_count * GROUPS
        hot[f] = (slots == group_ref[...] + place).astype(jnp.float32).astype(jnp.bfloat16)

    for f in range(freq_count):
        if f % per_load == 0:
            weight_copies[f // per_load].wait()
        loose[...] = weights[f].astype(jnp.float32)
        for j in range(halves):
            columns = pl.ds(j * LANES, LANES)
            for part in range(2):
                piece = loose[
                    pl.ds(2 * j + part, param_local, stride=2 * halves), :
                ].astype(jnp.bfloat16)
                dense[f, part, :, columns] = piece[:aligned]
                dense_tail[f % half_freqs, part, pl.ds(f // half_freqs * tail, tail), columns] = (
                    piece[aligned:]
                )

    mine = me_q * param_count + me_p
    ratio = math.sqrt(GROUPS / (gauge_local * qoi_count))

    def multiply(owners, f, chunk):
        if chunk < chunks:
            left = jnp.concatenate([line[chunk, q, f] for q in owners], axis=0)
            right = [dense[f, part, chunk * LANES : (chunk + 1) * LANES, :] for part in range(2)]
        else:
            left = jnp.concatenate([line_tail[q, f % half_freqs] for q in owners], axis=0)
            lane = lax.broadcasted_iota(jnp.int32, left.shape, 1)
            left = jnp.where((lane >= tail) == (f >= half_freqs), left.astype(jnp.float32), 0.0)
            left = left.astype(jnp.bfloat16)
            right = [dense_tail[f % half_freqs, part] for part in range(2)]
        real, imag = [jnp.dot(left, side, preferred_element_type=jnp.float32) for side in right]
        results = [[], []]
        for index in range(len(owners)):
            low, mid, high = [index * pair_rows + step * sample_local for step in range(3)]
            results[0].append(real[low:mid] - imag[mid:high])
            results[1].append(imag[low:mid] + real[mid:high])
        return [jnp.concatenate(result, axis=0) for result in results]

    def add_segment(segment, values, f):
        sums = lax.dot_general(
            jnp.concatenate(values, axis=0).astype(jnp.bfloat16),
            hot[f],
            NT_DIMS,
            preferred_element_type=jnp.float32,
        )
        return sums if segment is None else segment + sums

    def rows_of(k, f, count):
        return pl.ds((k * freq_count + f) * count, count)

    def deliver(owners, product, segment):
        count = len(owners) * sample_local
        joined[pl.ds(0, 2 * count), :] = segment * ratio
        for index, q in enumerate(owners):
            for i in range(sample_local):
                shares[q * sample_local + i] = joined[
                    pl.ds(index * sample_local + i, 2, stride=count), :
                ]
        for away in reversed(range(qoi_count)):
            for q in owners:
                for i in range(sample_local):
                    target = q * sample_local + i
                    copy = pltpu.make_async_remote_copy(
                        src_ref=shares.at[target],
                        dst_ref=gathered.at[mine],
                        send_sem=share_send,
                        recv_sem=share_recv,
                        device_id=(target, lax.rem(me_q + away, qoi_count)),
                        device_id_type=MESH,
                    )
                    if away:
                        copy.start()
                    else:
                        pl.when(target != me_p)(copy.start)
        for index, q in enumerate(owners):
            for i in range(sample_local):
                for j in range(halves):
                    outgoing[q * sample_local + i, :, j * LANES : (j + 1) * LANES] = product[
                        j, pl.ds(index * sample_local + i, stripe, stride=count), :
                    ].astype(jnp.bfloat16)
        for q in owners:
            for i in range(sample_local):
                target = q * sample_local + i
                copy = pltpu.make_async_remote_copy(
                    src_ref=outgoing.at[target],
                    dst_ref=incoming.at[me_p],
                    send_sem=out_send,
                    recv_sem=out_recv,
                    device_id=(target, me_q),
                    device_id_type=MESH,
                )
                pl.when(target != me_p)(copy.start)

    segment = None
    for f in range(freq_count):
        finals = [multiply([me_q], f, chunk) for chunk in range(chunks + 1)]
        values = [sum(pieces[1:], pieces[0]) for pieces in zip(*finals)]
        for k in range(2):
            for j in range(halves):
                near[j, rows_of(k, f, sample_local), :] = values[k][:, j * LANES : (j + 1) * LANES]
        segment = add_segment(segment, values, f)
    pl.semaphore_wait(known, len(contacts))
    deliver([me_q], near, segment)

    owners = [lax.rem(me_q + offset, qoi_count) for offset in range(1, qoi_count)]
    count = len(owners) * sample_local
    segment = None
    for chunk in range(chunks + 1):
        line_waits[chunk].wait_recv()
        for f in range(freq_count):
            values = multiply(owners, f, chunk)
            for k in range(2):
                wide = []
                for j in range(halves):
                    here = values[k][:, j * LANES : (j + 1) * LANES]
                    if chunk:
                        here = here + far[j, rows_of(k, f, count), :]
                    far[j, rows_of(k, f, count), :] = here
                    wide.append(here)
                values[k] = jnp.concatenate(wide, axis=1)
            if chunk == chunks:
                segment = add_segment(segment, values, f)
    deliver(owners, far, segment)
    incoming[me_p] = outgoing[me_p]
    gathered[mine] = shares[me_p]

    aside = (lax.rem(me_p + 1, param_count), me_q)
    others = incoming.at[pl.ds(0, param_count - 1)]
    out_wait = pltpu.make_async_remote_copy(
        src_ref=others, dst_ref=others, send_sem=out_send, recv_sem=out_recv,
        device_id=aside, device_id_type=MESH,
    )
    others = gathered.at[pl.ds(0, qoi_count * param_count - 1)]
    share_wait = pltpu.make_async_remote_copy(
        src_ref=others, dst_ref=others, send_sem=share_send, recv_sem=share_recv,
        device_id=aside, device_id_type=MESH,
    )
    out_wait.wait_recv()
    total = incoming[0].astype(jnp.float32)
    for p in range(1, param_count):
        total = total + incoming[p].astype(jnp.float32)
    out_ref[...] = total.reshape(out_ref.shape)
    share_wait.wait_recv()
    final = gathered[0]
    for p in range(1, param_count * qoi_count):
        final = final + gathered[p]
    for k in range(2):
        rows = jnp.broadcast_to(final[k : k + 1], (freq_count, LANES))
        turned = pltpu.roll(rows, 0, 1, stride=GROUPS, stride_axis=0)
        seg_ref[0, k] = turned[:, :GROUPS]
    for wait in line_waits:
        wait.wait_send()
    out_wait.wait_send()
    share_wait.wait_send()


def writer(spectrum_ref, response_ref, spectrum_hbm, response_hbm, sems):
    copies = [
        pltpu.make_async_copy(spectrum_ref, spectrum_hbm, sems.at[0]),
        pltpu.make_async_copy(response_ref, response_hbm, sems.at[1]),
    ]
    for copy in copies:
        copy.start()
    for copy in copies:
        copy.wait()


def local(samples, operator_rows, block_start, gauge_group):
    sample_local, param_local, steps_count = samples.shape
    freq_count, _, _, gauge_local = operator_rows.shape
    param_count, qoi_count = lax.axis_size("param"), lax.axis_size("qoi")
    sample_total = sample_local * qoi_count
    halves = gauge_local // LANES
    depth = 2 * param_local
    stripe = 2 * freq_count
    aligned = param_local // LANES * LANES
    tail = param_local - aligned
    assert sample_total == param_count and freq_count * GROUPS == LANES
    assert 2 * tail == LANES and freq_count % LOADS == 0 and steps_count % 2 == 0
    rows = operator_rows.reshape(freq_count, param_local, 2, halves, LANES)
    rows = rows.transpose(0, 1, 3, 2, 4).reshape(freq_count, depth * halves, LANES)
    dma = pltpu.SemaphoreType.DMA
    vmem = pl.BlockSpec(memory_space=pltpu.VMEM)
    hbm = pl.BlockSpec(memory_space=pltpu.HBM)
    shapes = (
        jax.ShapeDtypeStruct((1, 2, freq_count, gauge_local), jnp.float32),
        jax.ShapeDtypeStruct((1, 2, freq_count, GROUPS), jnp.float32),
    )
    found = pl.pallas_call(
        functools.partial(kernel, param_count, qoi_count),
        out_shape=shapes,
        in_specs=[pl.BlockSpec(memory_space=pltpu.SMEM), hbm, hbm, hbm],
        out_specs=(vmem, vmem),
        scratch_shapes=[
            pltpu.VMEM((1, gauge_local), jnp.int32),
            pltpu.VMEM((steps_count, sample_local, param_local), jnp.bfloat16),
            pltpu.VMEM((4 * freq_count * sample_local, steps_count // 2 * sample_local), jnp.bfloat16),
            pltpu.VMEM((freq_count, depth * halves, LANES), jnp.bfloat16),
            pltpu.VMEM((depth * halves, LANES), jnp.float32),
            pltpu.VMEM((freq_count, 2, aligned, gauge_local), jnp.bfloat16),
            pltpu.VMEM((freq_count // 2, 2, 2 * tail, gauge_local), jnp.bfloat16),
            pltpu.VMEM((freq_count, LANES, gauge_local), jnp.bfloat16),
            pltpu.VMEM((aligned // LANES, qoi_count, freq_count, 2 * sample_local, LANES), jnp.bfloat16),
            pltpu.VMEM((qoi_count, freq_count // 2, 2 * sample_local, 2 * tail), jnp.bfloat16),
            pltpu.VMEM((halves, stripe * sample_local, LANES), jnp.float32),
            pltpu.VMEM((halves, stripe * (sample_total - sample_local), LANES), jnp.float32),
            pltpu.VMEM((sample_total, stripe, gauge_local), jnp.bfloat16),
            pltpu.VMEM((param_count, stripe, gauge_local), jnp.bfloat16),
            pltpu.VMEM((2 * sample_total, LANES), jnp.float32),
            pltpu.VMEM((sample_total, 2, LANES), jnp.float32),
            pltpu.VMEM((qoi_count * param_count, 2, LANES), jnp.float32),
            dma(()),
            dma((2,)),
            dma((LOADS,)),
            dma((aligned // LANES + 1,)),
            dma((aligned // LANES + 1,)),
            dma(()),
            dma(()),
            dma(()),
            dma(()),
            pltpu.SemaphoreType.REGULAR,
        ],
        compiler_params=pltpu.CompilerParams(
            collective_id=0, has_side_effects=True, vmem_limit_bytes=53 * 2**20
        ),
    )(
        block_start,
        pltpu.with_memory_space_constraint(gauge_group.reshape(1, gauge_local), pltpu.HBM),
        samples.transpose(2, 0, 1),
        rows,
    )
    return pl.pallas_call(
        writer,
        out_shape=shapes,
        in_specs=[vmem, vmem],
        out_specs=(pl.BlockSpec(memory_space=pl.ANY), pl.BlockSpec(memory_space=pl.ANY)),
        scratch_shapes=[dma((2,))],
    )(*[pltpu.with_memory_space_constraint(array, pltpu.VMEM) for array in found])


def solution(mesh):
    return jax.shard_map(
        local,
        mesh=mesh,
        in_specs=(P("qoi", "param", None), P(None, "param", None, "qoi"), P(), P("qoi")),
        out_specs=(P("param", None, None, "qoi"), P("param", None, None, None)),
        check_vma=False,
    )
```

```python
import functools
import math

import jax
import jax.numpy as jnp
from jax import lax
from jax.experimental import pallas as pl
from jax.experimental.pallas import tpu as pltpu
from jax.sharding import PartitionSpec as P

GROUPS = 16
LANES = 128
LOADS = 2
MESH = pl.DeviceIdType.MESH
NT_DIMS = (((1,), (1,)), ((), ()))


def build_table(start, freq_count, steps_count, count, repeat, table):
    shape = (freq_count, count * repeat)
    steps = lax.broadcasted_iota(jnp.int32, shape, 1) // repeat
    freqs = lax.broadcasted_iota(jnp.int32, shape, 0) + start
    turns = (steps * freqs).astype(jnp.float32)
    whole = jnp.floor((turns + 0.5) * (1.0 / steps_count))
    phases = (turns - whole * steps_count) * (2.0 * math.pi / steps_count)
    scale = 1.0 / math.sqrt(steps_count)
    waves = [jnp.cos(phases) * scale, jnp.sin(phases) * -scale]
    highs = [wave.astype(jnp.bfloat16).astype(jnp.float32) for wave in waves]
    lows = [wave - high for wave, high in zip(waves, highs)]
    full = (repeat, count * repeat)
    keep = lax.broadcasted_iota(jnp.int32, full, 1) % repeat == lax.broadcasted_iota(
        jnp.int32, full, 0
    )
    for level, pair in enumerate((highs, lows)):
        for f in range(freq_count):
            rows = jnp.concatenate(
                [jnp.where(keep, jnp.broadcast_to(wave[f : f + 1], full), 0.0) for wave in pair],
                axis=0,
            )
            first = (level * freq_count + f) * 2 * repeat
            table[pl.ds(first, 2 * repeat), :] = rows.astype(jnp.bfloat16)


def kernel(
    param_count, qoi_count, start_ref, group_hbm, samples_hbm, rows_hbm,
    out_ref, seg_ref,
    group_ref, samples, table, weights, loose, dense, dense_tail, hot, line, near, far, outgoing, incoming, joined, shares, gathered,
    group_sem, samples_sem, weights_sem, line_send, line_recv, out_send, out_recv, share_send, share_recv, known,
):
    steps_count, sample_local, param_local = samples.shape
    freq_count = weights.shape[0]
    gauge_local = group_ref.shape[1]
    halves = gauge_local // LANES
    aligned = param_local // LANES * LANES
    tail = param_local - aligned
    chunks = aligned // LANES
    pair_rows = 2 * sample_local
    half_freqs = freq_count // 2
    half_steps = steps_count // 2
    stripe = 2 * freq_count
    inner = 2 ** (int(math.log2(param_count)) // 2)
    me_p = lax.axis_index("param")
    me_q = lax.axis_index("qoi")
    base = me_p // inner * inner

    contacts = []
    for turn in range(1, param_count // inner):
        contacts.append((lax.rem(me_p + turn * inner, param_count), me_q))
    for other in reversed(range(qoi_count)):
        for turn in range(inner):
            if other or turn:
                contacts.append(
                    (base + lax.rem(me_p + turn, inner), lax.rem(me_q + other, qoi_count))
                )
    barrier = pltpu.get_barrier_semaphore()
    sample_copy = pltpu.make_async_copy(samples_hbm, samples, samples_sem)
    sample_copy.start()
    for contact in contacts:
        pl.semaphore_signal(barrier, inc=1, device_id=contact, device_id_type=MESH)
    group_copy = pltpu.make_async_copy(group_hbm, group_ref, group_sem)
    group_copy.start()
    per_load = freq_count // LOADS
    loads = [pl.ds(load * per_load, per_load) for load in range(LOADS)]
    weight_copies = [
        pltpu.make_async_copy(rows_hbm.at[load], weights.at[load], weights_sem.at[index])
        for index, load in enumerate(loads)
    ]

    start = start_ref[0]
    build_table(start, freq_count, steps_count, half_steps, sample_local, table)

    group_copy.wait()
    slots = lax.broadcasted_iota(jnp.int32, (LANES, gauge_local), 0)
    for f in range(freq_count):
        place = (freq_count - f) % freq_count * GROUPS
        hot[f] = (slots == group_ref[...] + place).astype(jnp.float32).astype(jnp.bfloat16)

    sample_copy.wait()
    for copy in weight_copies:
        copy.start()
    pl.semaphore_wait(barrier, len(contacts))
    for contact in contacts:
        pl.semaphore_signal(known, inc=1, device_id=contact, device_id_type=MESH)

    def send_line(first, count, index):
        picked = pl.ds(first, count)
        for offset in range(1, qoi_count):
            pltpu.make_async_remote_copy(
                src_ref=line.at[me_q, picked],
                dst_ref=line.at[me_q, picked],
                send_sem=line_send,
                recv_sem=line_recv.at[index],
                device_id=(me_p, lax.rem(me_q + offset, qoi_count)),
                device_id_type=MESH,
            ).start()

    def wait_line(first, count, index):
        others = line.at[pl.ds(0, qoi_count - 1), pl.ds(first, count)]
        return pltpu.make_async_remote_copy(
            src_ref=others,
            dst_ref=others,
            send_sem=line_send,
            recv_sem=line_recv.at[index],
            device_id=(me_p, lax.rem(me_q + 1, qoi_count)),
            device_id_type=MESH,
        )

    turns = table[...]
    half = freq_count * pair_rows
    sides, ends = [], []
    for part in range(2):
        block = samples[pl.ds(part * half_steps, half_steps)]
        block = block.reshape(half_steps * sample_local, param_local)
        both = jnp.dot(turns, block[:, :aligned], preferred_element_type=jnp.float32)
        sides.append(both[:half] + both[half:])
        ends.append(block[:, aligned:])
    odd = lax.rem(start + lax.broadcasted_iota(jnp.int32, (half, LANES), 0) // pair_rows, 2)
    sign = 1.0 - 2.0 * odd.astype(jnp.float32)
    for chunk in range(chunks):
        columns = slice(chunk * LANES, (chunk + 1) * LANES)
        spectrum = sides[0][:, columns] + sign * sides[1][:, columns]
        line[me_q, chunk * freq_count : (chunk + 1) * freq_count] = spectrum.astype(
            jnp.bfloat16
        ).reshape(freq_count, pair_rows, LANES)
        send_line(chunk * freq_count, freq_count, chunk)
    both = jnp.dot(turns, jnp.concatenate(ends, axis=1), preferred_element_type=jnp.float32)
    both = both[:half] + both[half:]
    both = both + sign * pltpu.roll(both, tail, 1)
    middle = half // 2
    lane = lax.broadcasted_iota(jnp.int32, (middle, LANES), 1)
    packed = jnp.where(lane < tail, both[:middle], both[middle:] * sign[middle:])
    line[me_q, chunks * freq_count :] = packed.astype(jnp.bfloat16).reshape(
        half_freqs, pair_rows, LANES
    )
    send_line(chunks * freq_count, half_freqs, chunks)

    for f in range(freq_count):
        if f % per_load == 0:
            weight_copies[f // per_load].wait()
        loose[...] = weights[f].astype(jnp.float32)
        for j in range(halves):
            columns = pl.ds(j * LANES, LANES)
            for part in range(2):
                piece = loose[
                    pl.ds(2 * j + part, param_local, stride=2 * halves), :
                ].astype(jnp.bfloat16)
                dense[f, part, :, columns] = piece[:aligned]
                dense_tail[f % half_freqs, part, pl.ds(f // half_freqs * tail, tail), columns] = (
                    piece[aligned:]
                )

    mine = me_q * param_count + me_p
    ratio = math.sqrt(GROUPS / (gauge_local * qoi_count))

    def multiply(owners, f, chunk):
        if chunk < chunks:
            left = jnp.concatenate([line[q, chunk * freq_count + f] for q in owners], axis=0)
            right = [dense[f, part, chunk * LANES : (chunk + 1) * LANES, :] for part in range(2)]
        else:
            left = jnp.concatenate(
                [line[q, chunks * freq_count + f % half_freqs] for q in owners], axis=0
            )
            lane = lax.broadcasted_iota(jnp.int32, left.shape, 1)
            left = jnp.where((lane >= tail) == (f >= half_freqs), left.astype(jnp.float32), 0.0)
            left = left.astype(jnp.bfloat16)
            right = [dense_tail[f % half_freqs, part] for part in range(2)]
        real, imag = [jnp.dot(left, side, preferred_element_type=jnp.float32) for side in right]
        results = [[], []]
        for index in range(len(owners)):
            low, mid, high = [index * pair_rows + step * sample_local for step in range(3)]
            results[0].append(real[low:mid] - imag[mid:high])
            results[1].append(imag[low:mid] + real[mid:high])
        return [jnp.concatenate(result, axis=0) for result in results]

    def add_segment(segment, values, f):
        sums = lax.dot_general(
            jnp.concatenate(values, axis=0).astype(jnp.bfloat16),
            hot[f],
            NT_DIMS,
            preferred_element_type=jnp.float32,
        )
        return sums if segment is None else segment + sums

    def rows_of(k, f, count):
        return pl.ds((k * freq_count + f) * count, count)

    def deliver(owners, product, segment):
        count = len(owners) * sample_local
        joined[pl.ds(0, 2 * count), :] = segment * ratio
        for index, q in enumerate(owners):
            for i in range(sample_local):
                shares[q * sample_local + i] = joined[
                    pl.ds(index * sample_local + i, 2, stride=count), :
                ]
        for away in reversed(range(qoi_count)):
            for q in owners:
                for i in range(sample_local):
                    target = q * sample_local + i
                    copy = pltpu.make_async_remote_copy(
                        src_ref=shares.at[target],
                        dst_ref=gathered.at[mine],
                        send_sem=share_send,
                        recv_sem=share_recv,
                        device_id=(target, lax.rem(me_q + away, qoi_count)),
                        device_id_type=MESH,
                    )
                    if away:
                        copy.start()
                    else:
                        pl.when(target != me_p)(copy.start)
        for index, q in enumerate(owners):
            for i in range(sample_local):
                for j in range(halves):
                    outgoing[q * sample_local + i, :, j * LANES : (j + 1) * LANES] = product[
                        j, pl.ds(index * sample_local + i, stripe, stride=count), :
                    ].astype(jnp.bfloat16)
        for q in owners:
            for i in range(sample_local):
                target = q * sample_local + i
                copy = pltpu.make_async_remote_copy(
                    src_ref=outgoing.at[target],
                    dst_ref=incoming.at[me_p],
                    send_sem=out_send,
                    recv_sem=out_recv,
                    device_id=(target, me_q),
                    device_id_type=MESH,
                )
                pl.when(target != me_p)(copy.start)

    segment = None
    for f in range(freq_count):
        finals = [multiply([me_q], f, chunk) for chunk in range(chunks + 1)]
        values = [sum(pieces[1:], pieces[0]) for pieces in zip(*finals)]
        for k in range(2):
            for j in range(halves):
                near[j, rows_of(k, f, sample_local), :] = values[k][:, j * LANES : (j + 1) * LANES]
        segment = add_segment(segment, values, f)
    pl.semaphore_wait(known, len(contacts))
    deliver([me_q], near, segment)

    owners = [lax.rem(me_q + offset, qoi_count) for offset in range(1, qoi_count)]
    count = len(owners) * sample_local
    segment = None
    for chunk in range(chunks + 1):
        rows = freq_count if chunk < chunks else half_freqs
        wait_line(chunk * freq_count, rows, chunk).wait_recv()
        for f in range(freq_count):
            values = multiply(owners, f, chunk)
            for k in range(2):
                wide = []
                for j in range(halves):
                    here = values[k][:, j * LANES : (j + 1) * LANES]
                    if chunk:
                        here = here + far[j, rows_of(k, f, count), :]
                    far[j, rows_of(k, f, count), :] = here
                    wide.append(here)
                values[k] = jnp.concatenate(wide, axis=1)
            if chunk == chunks:
                segment = add_segment(segment, values, f)
    deliver(owners, far, segment)
    incoming[me_p] = outgoing[me_p]
    gathered[mine] = shares[me_p]

    aside = (lax.rem(me_p + 1, param_count), me_q)
    others = incoming.at[pl.ds(0, param_count - 1)]
    out_wait = pltpu.make_async_remote_copy(
        src_ref=others, dst_ref=others, send_sem=out_send, recv_sem=out_recv,
        device_id=aside, device_id_type=MESH,
    )
    others = gathered.at[pl.ds(0, qoi_count * param_count - 1)]
    share_wait = pltpu.make_async_remote_copy(
        src_ref=others, dst_ref=others, send_sem=share_send, recv_sem=share_recv,
        device_id=aside, device_id_type=MESH,
    )
    out_wait.wait_recv()
    total = incoming[0].astype(jnp.float32)
    for p in range(1, param_count):
        total = total + incoming[p].astype(jnp.float32)
    out_ref[...] = total.reshape(out_ref.shape)
    share_wait.wait_recv()
    final = gathered[0]
    for p in range(1, param_count * qoi_count):
        final = final + gathered[p]
    for k in range(2):
        rows = jnp.broadcast_to(final[k : k + 1], (freq_count, LANES))
        turned = pltpu.roll(rows, 0, 1, stride=GROUPS, stride_axis=0)
        seg_ref[0, k] = turned[:, :GROUPS]
    wait_line(0, chunks * freq_count + half_freqs, 0).wait_send()
    out_wait.wait_send()
    share_wait.wait_send()


def writer(spectrum_ref, response_ref, spectrum_hbm, response_hbm, sems):
    copies = [
        pltpu.make_async_copy(spectrum_ref, spectrum_hbm, sems.at[0]),
        pltpu.make_async_copy(response_ref, response_hbm, sems.at[1]),
    ]
    for copy in copies:
        copy.start()
    for copy in copies:
        copy.wait()


def local(samples, operator_rows, block_start, gauge_group):
    sample_local, param_local, steps_count = samples.shape
    freq_count, _, _, gauge_local = operator_rows.shape
    param_count, qoi_count = lax.axis_size("param"), lax.axis_size("qoi")
    sample_total = sample_local * qoi_count
    halves = gauge_local // LANES
    depth = 2 * param_local
    stripe = 2 * freq_count
    aligned = param_local // LANES * LANES
    tail = param_local - aligned
    assert sample_total == param_count and freq_count * GROUPS == LANES
    assert 2 * tail == LANES and freq_count % LOADS == 0 and steps_count % 2 == 0
    rows = operator_rows.reshape(freq_count, param_local, 2, halves, LANES)
    rows = rows.transpose(0, 1, 3, 2, 4).reshape(freq_count, depth * halves, LANES)
    dma = pltpu.SemaphoreType.DMA
    vmem = pl.BlockSpec(memory_space=pltpu.VMEM)
    hbm = pl.BlockSpec(memory_space=pltpu.HBM)
    shapes = (
        jax.ShapeDtypeStruct((1, 2, freq_count, gauge_local), jnp.float32),
        jax.ShapeDtypeStruct((1, 2, freq_count, GROUPS), jnp.float32),
    )
    found = pl.pallas_call(
        functools.partial(kernel, param_count, qoi_count),
        out_shape=shapes,
        in_specs=[pl.BlockSpec(memory_space=pltpu.SMEM), hbm, hbm, hbm],
        out_specs=(vmem, vmem),
        scratch_shapes=[
            pltpu.VMEM((1, gauge_local), jnp.int32),
            pltpu.VMEM((steps_count, sample_local, param_local), jnp.bfloat16),
            pltpu.VMEM((4 * freq_count * sample_local, steps_count // 2 * sample_local), jnp.bfloat16),
            pltpu.VMEM((freq_count, depth * halves, LANES), jnp.bfloat16),
            pltpu.VMEM((depth * halves, LANES), jnp.float32),
            pltpu.VMEM((freq_count, 2, aligned, gauge_local), jnp.bfloat16),
            pltpu.VMEM((freq_count // 2, 2, 2 * tail, gauge_local), jnp.bfloat16),
            pltpu.VMEM((freq_count, LANES, gauge_local), jnp.bfloat16),
            pltpu.VMEM(
                (qoi_count, aligned // LANES * freq_count + freq_count // 2, 2 * sample_local, LANES),
                jnp.bfloat16,
            ),
            pltpu.VMEM((halves, stripe * sample_local, LANES), jnp.float32),
            pltpu.VMEM((halves, stripe * (sample_total - sample_local), LANES), jnp.float32),
            pltpu.VMEM((sample_total, stripe, gauge_local), jnp.bfloat16),
            pltpu.VMEM((param_count, stripe, gauge_local), jnp.bfloat16),
            pltpu.VMEM((2 * sample_total, LANES), jnp.float32),
            pltpu.VMEM((sample_total, 2, LANES), jnp.float32),
            pltpu.VMEM((qoi_count * param_count, 2, LANES), jnp.float32),
            dma(()),
            dma(()),
            dma((LOADS,)),
            dma(()),
            dma((aligned // LANES + 1,)),
            dma(()),
            dma(()),
            dma(()),
            dma(()),
            pltpu.SemaphoreType.REGULAR,
        ],
        compiler_params=pltpu.CompilerParams(
            collective_id=0, has_side_effects=True, vmem_limit_bytes=53 * 2**20
        ),
    )(
        block_start,
        pltpu.with_memory_space_constraint(gauge_group.reshape(1, gauge_local), pltpu.HBM),
        samples.transpose(2, 0, 1),
        rows,
    )
    return pl.pallas_call(
        writer,
        out_shape=shapes,
        in_specs=[vmem, vmem],
        out_specs=(pl.BlockSpec(memory_space=pl.ANY), pl.BlockSpec(memory_space=pl.ANY)),
        scratch_shapes=[dma((2,))],
    )(*[pltpu.with_memory_space_constraint(array, pltpu.VMEM) for array in found])


def solution(mesh):
    return jax.shard_map(
        local,
        mesh=mesh,
        in_specs=(P("qoi", "param", None), P(None, "param", None, "qoi"), P(), P("qoi")),
        out_specs=(P("param", None, None, "qoi"), P("param", None, None, None)),
        check_vma=False,
    )
```

```python
import functools
import math

import jax
import jax.numpy as jnp
from jax import lax
from jax.experimental import pallas as pl
from jax.experimental.pallas import tpu as pltpu
from jax.sharding import PartitionSpec as P

GROUPS = 16
LANES = 128
LOADS = 2
MESH = pl.DeviceIdType.MESH
NT_DIMS = (((1,), (1,)), ((), ()))


def build_table(start, freq_count, steps_count, count, repeat, table):
    shape = (freq_count, count * repeat)
    steps = lax.broadcasted_iota(jnp.int32, shape, 1) // repeat
    freqs = lax.broadcasted_iota(jnp.int32, shape, 0) + start
    turns = (steps * freqs).astype(jnp.float32)
    whole = jnp.floor((turns + 0.5) * (1.0 / steps_count))
    phases = (turns - whole * steps_count) * (2.0 * math.pi / steps_count)
    scale = 1.0 / math.sqrt(steps_count)
    waves = [jnp.cos(phases) * scale, jnp.sin(phases) * -scale]
    highs = [wave.astype(jnp.bfloat16).astype(jnp.float32) for wave in waves]
    lows = [wave - high for wave, high in zip(waves, highs)]
    full = (repeat, count * repeat)
    keep = lax.broadcasted_iota(jnp.int32, full, 1) % repeat == lax.broadcasted_iota(
        jnp.int32, full, 0
    )
    for level, pair in enumerate((highs, lows)):
        for f in range(freq_count):
            rows = jnp.concatenate(
                [jnp.where(keep, jnp.broadcast_to(wave[f : f + 1], full), 0.0) for wave in pair],
                axis=0,
            )
            first = (level * freq_count + f) * 2 * repeat
            table[pl.ds(first, 2 * repeat), :] = rows.astype(jnp.bfloat16)


def kernel(
    param_count, qoi_count, start_ref, group_hbm, samples_hbm, rows_hbm,
    out_ref, seg_ref,
    group_ref, samples, table, weights, loose, dense, dense_tail, hot, line, near, far, outgoing, incoming, joined, shares, gathered,
    group_sem, samples_sem, weights_sem, line_send, line_recv, out_send, out_recv, share_send, share_recv, known,
):
    steps_count, sample_local, param_local = samples.shape
    freq_count = weights.shape[0]
    gauge_local = group_ref.shape[1]
    halves = gauge_local // LANES
    aligned = param_local // LANES * LANES
    tail = param_local - aligned
    chunks = aligned // LANES
    pair_rows = 2 * sample_local
    half_freqs = freq_count // 2
    half_steps = steps_count // 2
    stripe = 2 * freq_count
    inner = 2 ** (int(math.log2(param_count)) // 2)
    me_p = lax.axis_index("param")
    me_q = lax.axis_index("qoi")
    base = me_p // inner * inner

    contacts = []
    for turn in range(1, param_count // inner):
        contacts.append((lax.rem(me_p + turn * inner, param_count), me_q))
    for other in reversed(range(qoi_count)):
        for turn in range(inner):
            if other or turn:
                contacts.append(
                    (base + lax.rem(me_p + turn, inner), lax.rem(me_q + other, qoi_count))
                )
    barrier = pltpu.get_barrier_semaphore()
    group_copy = pltpu.make_async_copy(group_hbm, group_ref, group_sem)
    group_copy.start()
    sample_copy = pltpu.make_async_copy(samples_hbm, samples, samples_sem)
    sample_copy.start()
    for contact in contacts:
        pl.semaphore_signal(barrier, inc=1, device_id=contact, device_id_type=MESH)
    per_load = freq_count // LOADS
    loads = [pl.ds(load * per_load, per_load) for load in range(LOADS)]
    weight_copies = [
        pltpu.make_async_copy(rows_hbm.at[load], weights.at[load], weights_sem.at[index])
        for index, load in enumerate(loads)
    ]

    start = start_ref[0]
    build_table(start, freq_count, steps_count, half_steps, sample_local, table)
    for copy in weight_copies:
        copy.start()

    group_copy.wait()
    slots = lax.broadcasted_iota(jnp.int32, (LANES, gauge_local), 0)
    for f in range(freq_count):
        place = (freq_count - f) % freq_count * GROUPS
        hot[f] = (slots == group_ref[...] + place).astype(jnp.float32).astype(jnp.bfloat16)

    sample_copy.wait()

    def send_line(first, count, index):
        picked = pl.ds(first, count)
        for offset in range(1, qoi_count):
            pltpu.make_async_remote_copy(
                src_ref=line.at[me_q, picked],
                dst_ref=line.at[me_q, picked],
                send_sem=line_send,
                recv_sem=line_recv.at[index],
                device_id=(me_p, lax.rem(me_q + offset, qoi_count)),
                device_id_type=MESH,
            ).start()

    def wait_line(first, count, index):
        others = line.at[pl.ds(0, qoi_count - 1), pl.ds(first, count)]
        return pltpu.make_async_remote_copy(
            src_ref=others,
            dst_ref=others,
            send_sem=line_send,
            recv_sem=line_recv.at[index],
            device_id=(me_p, lax.rem(me_q + 1, qoi_count)),
            device_id_type=MESH,
        )

    turns = table[...]
    half = freq_count * pair_rows
    sides, ends = [], []
    for part in range(2):
        block = samples[pl.ds(part * half_steps, half_steps)]
        block = block.reshape(half_steps * sample_local, param_local)
        both = jnp.dot(turns, block[:, :aligned], preferred_element_type=jnp.float32)
        sides.append(both[:half] + both[half:])
        ends.append(block[:, aligned:])
    odd = lax.rem(start + lax.broadcasted_iota(jnp.int32, (half, LANES), 0) // pair_rows, 2)
    sign = 1.0 - 2.0 * odd.astype(jnp.float32)
    pl.semaphore_wait(barrier, len(contacts))
    for chunk in range(chunks):
        columns = slice(chunk * LANES, (chunk + 1) * LANES)
        spectrum = sides[0][:, columns] + sign * sides[1][:, columns]
        line[me_q, chunk * freq_count : (chunk + 1) * freq_count] = spectrum.astype(
            jnp.bfloat16
        ).reshape(freq_count, pair_rows, LANES)
        send_line(chunk * freq_count, freq_count, chunk)
    for contact in contacts:
        pl.semaphore_signal(known, inc=1, device_id=contact, device_id_type=MESH)
    both = jnp.dot(turns, jnp.concatenate(ends, axis=1), preferred_element_type=jnp.float32)
    both = both[:half] + both[half:]
    both = both + sign * pltpu.roll(both, tail, 1)
    middle = half // 2
    lane = lax.broadcasted_iota(jnp.int32, (middle, LANES), 1)
    packed = jnp.where(lane < tail, both[:middle], both[middle:] * sign[middle:])
    line[me_q, chunks * freq_count :] = packed.astype(jnp.bfloat16).reshape(
        half_freqs, pair_rows, LANES
    )
    send_line(chunks * freq_count, half_freqs, chunks)

    for f in range(freq_count):
        if f % per_load == 0:
            weight_copies[f // per_load].wait()
        loose[...] = weights[f].astype(jnp.float32)
        for j in range(halves):
            columns = pl.ds(j * LANES, LANES)
            for part in range(2):
                piece = loose[
                    pl.ds(2 * j + part, param_local, stride=2 * halves), :
                ].astype(jnp.bfloat16)
                dense[f, part, :, columns] = piece[:aligned]
                dense_tail[f % half_freqs, part, pl.ds(f // half_freqs * tail, tail), columns] = (
                    piece[aligned:]
                )

    mine = me_q * param_count + me_p
    ratio = math.sqrt(GROUPS / (gauge_local * qoi_count))

    def multiply(owners, f, chunk):
        if chunk < chunks:
            left = jnp.concatenate([line[q, chunk * freq_count + f] for q in owners], axis=0)
            right = [dense[f, part, chunk * LANES : (chunk + 1) * LANES, :] for part in range(2)]
        else:
            left = jnp.concatenate(
                [line[q, chunks * freq_count + f % half_freqs] for q in owners], axis=0
            )
            lane = lax.broadcasted_iota(jnp.int32, left.shape, 1)
            left = jnp.where((lane >= tail) == (f >= half_freqs), left.astype(jnp.float32), 0.0)
            left = left.astype(jnp.bfloat16)
            right = [dense_tail[f % half_freqs, part] for part in range(2)]
        real, imag = [jnp.dot(left, side, preferred_element_type=jnp.float32) for side in right]
        results = [[], []]
        for index in range(len(owners)):
            low, mid, high = [index * pair_rows + step * sample_local for step in range(3)]
            results[0].append(real[low:mid] - imag[mid:high])
            results[1].append(imag[low:mid] + real[mid:high])
        return [jnp.concatenate(result, axis=0) for result in results]

    def add_segment(segment, values, f):
        sums = lax.dot_general(
            jnp.concatenate(values, axis=0).astype(jnp.bfloat16),
            hot[f],
            NT_DIMS,
            preferred_element_type=jnp.float32,
        )
        return sums if segment is None else segment + sums

    def rows_of(k, f, count):
        return pl.ds((k * freq_count + f) * count, count)

    def deliver(owners, product, segment):
        count = len(owners) * sample_local
        joined[pl.ds(0, 2 * count), :] = segment * ratio
        for index, q in enumerate(owners):
            for i in range(sample_local):
                shares[q * sample_local + i] = joined[
                    pl.ds(index * sample_local + i, 2, stride=count), :
                ]
        for away in reversed(range(qoi_count)):
            for q in owners:
                for i in range(sample_local):
                    target = q * sample_local + i
                    copy = pltpu.make_async_remote_copy(
                        src_ref=shares.at[target],
                        dst_ref=gathered.at[mine],
                        send_sem=share_send,
                        recv_sem=share_recv,
                        device_id=(target, lax.rem(me_q + away, qoi_count)),
                        device_id_type=MESH,
                    )
                    if away:
                        copy.start()
                    else:
                        pl.when(target != me_p)(copy.start)
        for index, q in enumerate(owners):
            for i in range(sample_local):
                for j in range(halves):
                    outgoing[q * sample_local + i, :, j * LANES : (j + 1) * LANES] = product[
                        j, pl.ds(index * sample_local + i, stripe, stride=count), :
                    ].astype(jnp.bfloat16)
        for q in owners:
            for i in range(sample_local):
                target = q * sample_local + i
                copy = pltpu.make_async_remote_copy(
                    src_ref=outgoing.at[target],
                    dst_ref=incoming.at[me_p],
                    send_sem=out_send,
                    recv_sem=out_recv,
                    device_id=(target, me_q),
                    device_id_type=MESH,
                )
                pl.when(target != me_p)(copy.start)

    for owners, product in (([0], near), (list(range(1, qoi_count)), far)):
        count = len(owners) * sample_local
        segment = None
        for chunk in range(chunks + 1):
            rows = freq_count if chunk < chunks else half_freqs
            line_wait = wait_line(chunk * freq_count, rows, chunk)
            pl.when(me_q != 0 if owners == [0] else me_q == 0)(line_wait.wait_recv)
            for f in range(freq_count):
                values = multiply(owners, f, chunk)
                for k in range(2):
                    wide = []
                    for j in range(halves):
                        here = values[k][:, j * LANES : (j + 1) * LANES]
                        if chunk:
                            here = here + product[j, rows_of(k, f, count), :]
                        product[j, rows_of(k, f, count), :] = here
                        wide.append(here)
                    values[k] = jnp.concatenate(wide, axis=1)
                if chunk == chunks:
                    segment = add_segment(segment, values, f)
        if owners == [0]:
            pl.semaphore_wait(known, len(contacts))
        deliver(owners, product, segment)
    incoming[me_p] = outgoing[me_p]
    gathered[mine] = shares[me_p]

    aside = (lax.rem(me_p + 1, param_count), me_q)
    others = incoming.at[pl.ds(0, param_count - 1)]
    out_wait = pltpu.make_async_remote_copy(
        src_ref=others, dst_ref=others, send_sem=out_send, recv_sem=out_recv,
        device_id=aside, device_id_type=MESH,
    )
    others = gathered.at[pl.ds(0, qoi_count * param_count - 1)]
    share_wait = pltpu.make_async_remote_copy(
        src_ref=others, dst_ref=others, send_sem=share_send, recv_sem=share_recv,
        device_id=aside, device_id_type=MESH,
    )
    out_wait.wait_recv()
    total = incoming[0].astype(jnp.float32)
    for p in range(1, param_count):
        total = total + incoming[p].astype(jnp.float32)
    out_ref[...] = total.reshape(out_ref.shape)
    share_wait.wait_recv()
    final = gathered[0]
    for p in range(1, param_count * qoi_count):
        final = final + gathered[p]
    for k in range(2):
        rows = jnp.broadcast_to(final[k : k + 1], (freq_count, LANES))
        turned = pltpu.roll(rows, 0, 1, stride=GROUPS, stride_axis=0)
        seg_ref[0, k] = turned[:, :GROUPS]
    wait_line(0, chunks * freq_count + half_freqs, 0).wait_send()
    out_wait.wait_send()
    share_wait.wait_send()


def writer(spectrum_ref, response_ref, spectrum_hbm, response_hbm, sems):
    copies = [
        pltpu.make_async_copy(spectrum_ref, spectrum_hbm, sems.at[0]),
        pltpu.make_async_copy(response_ref, response_hbm, sems.at[1]),
    ]
    for copy in copies:
        copy.start()
    for copy in copies:
        copy.wait()


def local(samples, operator_rows, block_start, gauge_group):
    sample_local, param_local, steps_count = samples.shape
    freq_count, _, _, gauge_local = operator_rows.shape
    param_count, qoi_count = lax.axis_size("param"), lax.axis_size("qoi")
    sample_total = sample_local * qoi_count
    halves = gauge_local // LANES
    depth = 2 * param_local
    stripe = 2 * freq_count
    aligned = param_local // LANES * LANES
    tail = param_local - aligned
    assert sample_total == param_count and freq_count * GROUPS == LANES
    assert 2 * tail == LANES and freq_count % LOADS == 0 and steps_count % 2 == 0
    rows = operator_rows.reshape(freq_count, param_local, 2, halves, LANES)
    rows = rows.transpose(0, 1, 3, 2, 4).reshape(freq_count, depth * halves, LANES)
    dma = pltpu.SemaphoreType.DMA
    vmem = pl.BlockSpec(memory_space=pltpu.VMEM)
    hbm = pl.BlockSpec(memory_space=pltpu.HBM)
    shapes = (
        jax.ShapeDtypeStruct((1, 2, freq_count, gauge_local), jnp.float32),
        jax.ShapeDtypeStruct((1, 2, freq_count, GROUPS), jnp.float32),
    )
    found = pl.pallas_call(
        functools.partial(kernel, param_count, qoi_count),
        out_shape=shapes,
        in_specs=[pl.BlockSpec(memory_space=pltpu.SMEM), hbm, hbm, hbm],
        out_specs=(vmem, vmem),
        scratch_shapes=[
            pltpu.VMEM((1, gauge_local), jnp.int32),
            pltpu.VMEM((steps_count, sample_local, param_local), jnp.bfloat16),
            pltpu.VMEM((4 * freq_count * sample_local, steps_count // 2 * sample_local), jnp.bfloat16),
            pltpu.VMEM((freq_count, depth * halves, LANES), jnp.bfloat16),
            pltpu.VMEM((depth * halves, LANES), jnp.float32),
            pltpu.VMEM((freq_count, 2, aligned, gauge_local), jnp.bfloat16),
            pltpu.VMEM((freq_count // 2, 2, 2 * tail, gauge_local), jnp.bfloat16),
            pltpu.VMEM((freq_count, LANES, gauge_local), jnp.bfloat16),
            pltpu.VMEM(
                (qoi_count, aligned // LANES * freq_count + freq_count // 2, 2 * sample_local, LANES),
                jnp.bfloat16,
            ),
            pltpu.VMEM((halves, stripe * sample_local, LANES), jnp.float32),
            pltpu.VMEM((halves, stripe * (sample_total - sample_local), LANES), jnp.float32),
            pltpu.VMEM((sample_total, stripe, gauge_local), jnp.bfloat16),
            pltpu.VMEM((param_count, stripe, gauge_local), jnp.bfloat16),
            pltpu.VMEM((2 * sample_total, LANES), jnp.float32),
            pltpu.VMEM((sample_total, 2, LANES), jnp.float32),
            pltpu.VMEM((qoi_count * param_count, 2, LANES), jnp.float32),
            dma(()),
            dma(()),
            dma((LOADS,)),
            dma(()),
            dma((aligned // LANES + 1,)),
            dma(()),
            dma(()),
            dma(()),
            dma(()),
            pltpu.SemaphoreType.REGULAR,
        ],
        compiler_params=pltpu.CompilerParams(
            collective_id=0, has_side_effects=True, vmem_limit_bytes=53 * 2**20
        ),
    )(
        block_start,
        pltpu.with_memory_space_constraint(gauge_group.reshape(1, gauge_local), pltpu.HBM),
        samples.transpose(2, 0, 1),
        rows,
    )
    return pl.pallas_call(
        writer,
        out_shape=shapes,
        in_specs=[vmem, vmem],
        out_specs=(pl.BlockSpec(memory_space=pl.ANY), pl.BlockSpec(memory_space=pl.ANY)),
        scratch_shapes=[dma((2,))],
    )(*[pltpu.with_memory_space_constraint(array, pltpu.VMEM) for array in found])


def solution(mesh):
    return jax.shard_map(
        local,
        mesh=mesh,
        in_specs=(P("qoi", "param", None), P(None, "param", None, "qoi"), P(), P("qoi")),
        out_specs=(P("param", None, None, "qoi"), P("param", None, None, None)),
        check_vma=False,
    )
```

```python
import functools
import math

import jax
import jax.numpy as jnp
from jax import lax
from jax.experimental import pallas as pl
from jax.experimental.pallas import tpu as pltpu
from jax.sharding import PartitionSpec as P

GROUPS = 16
LANES = 128
LOADS = 2
MESH = pl.DeviceIdType.MESH
NT_DIMS = (((1,), (1,)), ((), ()))


def build_table(start, freq_count, steps_count, count, repeat, table):
    shape = (freq_count, count * repeat)
    steps = lax.broadcasted_iota(jnp.int32, shape, 1) // repeat
    freqs = lax.broadcasted_iota(jnp.int32, shape, 0) + start
    turns = (steps * freqs).astype(jnp.float32)
    whole = jnp.floor((turns + 0.5) * (1.0 / steps_count))
    phases = (turns - whole * steps_count) * (2.0 * math.pi / steps_count)
    scale = 1.0 / math.sqrt(steps_count)
    waves = [jnp.cos(phases) * scale, jnp.sin(phases) * -scale]
    highs = [wave.astype(jnp.bfloat16).astype(jnp.float32) for wave in waves]
    lows = [wave - high for wave, high in zip(waves, highs)]
    full = (repeat, count * repeat)
    keep = lax.broadcasted_iota(jnp.int32, full, 1) % repeat == lax.broadcasted_iota(
        jnp.int32, full, 0
    )
    for level, pair in enumerate((highs, lows)):
        for f in range(freq_count):
            rows = jnp.concatenate(
                [jnp.where(keep, jnp.broadcast_to(wave[f : f + 1], full), 0.0) for wave in pair],
                axis=0,
            )
            first = (level * freq_count + f) * 2 * repeat
            table[pl.ds(first, 2 * repeat), :] = rows.astype(jnp.bfloat16)


def kernel(
    param_count, qoi_count, start_ref, group_hbm, samples_hbm, rows_hbm,
    out_ref, seg_ref,
    group_ref, samples, table, weights, loose, dense, dense_tail, hot, line, near, far, outgoing, incoming, joined, shares, gathered,
    group_sem, samples_sem, weights_sem, line_send, line_recv, out_send, out_recv, share_send, share_recv, known,
):
    steps_count, sample_local, param_local = samples.shape
    freq_count = weights.shape[0]
    gauge_local = group_ref.shape[1]
    halves = gauge_local // LANES
    aligned = param_local // LANES * LANES
    tail = param_local - aligned
    chunks = aligned // LANES
    pair_rows = 2 * sample_local
    half_freqs = freq_count // 2
    half_steps = steps_count // 2
    stripe = 2 * freq_count
    inner = 2 ** (int(math.log2(param_count)) // 2)
    me_p = lax.axis_index("param")
    me_q = lax.axis_index("qoi")
    base = me_p // inner * inner

    contacts = []
    for turn in range(1, param_count // inner):
        contacts.append((lax.rem(me_p + turn * inner, param_count), me_q))
    for other in reversed(range(qoi_count)):
        for turn in range(inner):
            if other or turn:
                contacts.append(
                    (base + lax.rem(me_p + turn, inner), lax.rem(me_q + other, qoi_count))
                )
    barrier = pltpu.get_barrier_semaphore()
    group_copy = pltpu.make_async_copy(group_hbm, group_ref, group_sem)
    group_copy.start()
    lanes = [pl.ds(0, aligned), pl.ds(aligned, tail)]
    sample_copies = [
        pltpu.make_async_copy(samples_hbm.at[:, :, lane], samples.at[:, :, lane], samples_sem.at[part])
        for part, lane in enumerate(lanes)
    ]
    for copy in sample_copies:
        copy.start()
    for contact in contacts:
        pl.semaphore_signal(barrier, inc=1, device_id=contact, device_id_type=MESH)
    per_load = freq_count // LOADS
    loads = [pl.ds(load * per_load, per_load) for load in range(LOADS)]
    weight_copies = [
        pltpu.make_async_copy(rows_hbm.at[load], weights.at[load], weights_sem.at[index])
        for index, load in enumerate(loads)
    ]

    start = start_ref[0]
    build_table(start, freq_count, steps_count, half_steps, sample_local, table)
    for copy in weight_copies:
        copy.start()

    sample_copies[0].wait()

    def send_line(first, count, index):
        picked = pl.ds(first, count)
        for offset in range(1, qoi_count):
            pltpu.make_async_remote_copy(
                src_ref=line.at[me_q, picked],
                dst_ref=line.at[me_q, picked],
                send_sem=line_send,
                recv_sem=line_recv.at[index],
                device_id=(me_p, lax.rem(me_q + offset, qoi_count)),
                device_id_type=MESH,
            ).start()

    def wait_line(first, count, index):
        others = line.at[pl.ds(0, qoi_count - 1), pl.ds(first, count)]
        return pltpu.make_async_remote_copy(
            src_ref=others,
            dst_ref=others,
            send_sem=line_send,
            recv_sem=line_recv.at[index],
            device_id=(me_p, lax.rem(me_q + 1, qoi_count)),
            device_id_type=MESH,
        )

    turns = table[...]
    half = freq_count * pair_rows
    sides, ends = [], []
    for part in range(2):
        block = samples[pl.ds(part * half_steps, half_steps), :, pl.ds(0, aligned)]
        block = block.reshape(half_steps * sample_local, aligned)
        both = jnp.dot(turns, block, preferred_element_type=jnp.float32)
        sides.append(both[:half] + both[half:])
    odd = lax.rem(start + lax.broadcasted_iota(jnp.int32, (half, LANES), 0) // pair_rows, 2)
    sign = 1.0 - 2.0 * odd.astype(jnp.float32)
    pl.semaphore_wait(barrier, len(contacts))
    for chunk in range(chunks):
        columns = slice(chunk * LANES, (chunk + 1) * LANES)
        spectrum = sides[0][:, columns] + sign * sides[1][:, columns]
        line[me_q, chunk * freq_count : (chunk + 1) * freq_count] = spectrum.astype(
            jnp.bfloat16
        ).reshape(freq_count, pair_rows, LANES)
        send_line(chunk * freq_count, freq_count, chunk)
    for contact in contacts:
        pl.semaphore_signal(known, inc=1, device_id=contact, device_id_type=MESH)
    sample_copies[1].wait()
    for part in range(2):
        block = samples[pl.ds(part * half_steps, half_steps), :, pl.ds(aligned, tail)]
        ends.append(block.reshape(half_steps * sample_local, tail))
    both = jnp.dot(turns, jnp.concatenate(ends, axis=1), preferred_element_type=jnp.float32)
    both = both[:half] + both[half:]
    both = both + sign * pltpu.roll(both, tail, 1)
    middle = half // 2
    lane = lax.broadcasted_iota(jnp.int32, (middle, LANES), 1)
    packed = jnp.where(lane < tail, both[:middle], both[middle:] * sign[middle:])
    line[me_q, chunks * freq_count :] = packed.astype(jnp.bfloat16).reshape(
        half_freqs, pair_rows, LANES
    )
    send_line(chunks * freq_count, half_freqs, chunks)

    group_copy.wait()
    slots = lax.broadcasted_iota(jnp.int32, (LANES, gauge_local), 0)
    for f in range(freq_count):
        place = (freq_count - f) % freq_count * GROUPS
        hot[f] = (slots == group_ref[...] + place).astype(jnp.float32).astype(jnp.bfloat16)

    for f in range(freq_count):
        if f % per_load == 0:
            weight_copies[f // per_load].wait()
        loose[...] = weights[f].astype(jnp.float32)
        for j in range(halves):
            columns = pl.ds(j * LANES, LANES)
            for part in range(2):
                piece = loose[
                    pl.ds(2 * j + part, param_local, stride=2 * halves), :
                ].astype(jnp.bfloat16)
                dense[f, part, :, columns] = piece[:aligned]
                dense_tail[f % half_freqs, part, pl.ds(f // half_freqs * tail, tail), columns] = (
                    piece[aligned:]
                )

    mine = me_q * param_count + me_p
    ratio = math.sqrt(GROUPS / (gauge_local * qoi_count))

    def multiply(owners, f, chunk):
        if chunk < chunks:
            left = jnp.concatenate([line[q, chunk * freq_count + f] for q in owners], axis=0)
            right = [dense[f, part, chunk * LANES : (chunk + 1) * LANES, :] for part in range(2)]
        else:
            left = jnp.concatenate(
                [line[q, chunks * freq_count + f % half_freqs] for q in owners], axis=0
            )
            lane = lax.broadcasted_iota(jnp.int32, left.shape, 1)
            left = jnp.where((lane >= tail) == (f >= half_freqs), left.astype(jnp.float32), 0.0)
            left = left.astype(jnp.bfloat16)
            right = [dense_tail[f % half_freqs, part] for part in range(2)]
        real, imag = [jnp.dot(left, side, preferred_element_type=jnp.float32) for side in right]
        results = [[], []]
        for index in range(len(owners)):
            low, mid, high = [index * pair_rows + step * sample_local for step in range(3)]
            results[0].append(real[low:mid] - imag[mid:high])
            results[1].append(imag[low:mid] + real[mid:high])
        return [jnp.concatenate(result, axis=0) for result in results]

    def add_segment(segment, values, f):
        sums = lax.dot_general(
            jnp.concatenate(values, axis=0).astype(jnp.bfloat16),
            hot[f],
            NT_DIMS,
            preferred_element_type=jnp.float32,
        )
        return sums if segment is None else segment + sums

    def rows_of(k, f, count):
        return pl.ds((k * freq_count + f) * count, count)

    def deliver(owners, product, segment):
        count = len(owners) * sample_local
        joined[pl.ds(0, 2 * count), :] = segment * ratio
        for index, q in enumerate(owners):
            for i in range(sample_local):
                shares[q * sample_local + i] = joined[
                    pl.ds(index * sample_local + i, 2, stride=count), :
                ]
        for away in reversed(range(qoi_count)):
            for q in owners:
                for i in range(sample_local):
                    target = q * sample_local + i
                    copy = pltpu.make_async_remote_copy(
                        src_ref=shares.at[target],
                        dst_ref=gathered.at[mine],
                        send_sem=share_send,
                        recv_sem=share_recv,
                        device_id=(target, lax.rem(me_q + away, qoi_count)),
                        device_id_type=MESH,
                    )
                    if away:
                        copy.start()
                    else:
                        pl.when(target != me_p)(copy.start)
        for index, q in enumerate(owners):
            for i in range(sample_local):
                for j in range(halves):
                    outgoing[q * sample_local + i, :, j * LANES : (j + 1) * LANES] = product[
                        j, pl.ds(index * sample_local + i, stripe, stride=count), :
                    ].astype(jnp.bfloat16)
        for q in owners:
            for i in range(sample_local):
                target = q * sample_local + i
                copy = pltpu.make_async_remote_copy(
                    src_ref=outgoing.at[target],
                    dst_ref=incoming.at[me_p],
                    send_sem=out_send,
                    recv_sem=out_recv,
                    device_id=(target, me_q),
                    device_id_type=MESH,
                )
                pl.when(target != me_p)(copy.start)

    for owners, product in (([0], near), (list(range(1, qoi_count)), far)):
        count = len(owners) * sample_local
        segment = None
        for chunk in range(chunks + 1):
            rows = freq_count if chunk < chunks else half_freqs
            line_wait = wait_line(chunk * freq_count, rows, chunk)
            pl.when(me_q != 0 if owners == [0] else me_q == 0)(line_wait.wait_recv)
            for f in range(freq_count):
                values = multiply(owners, f, chunk)
                for k in range(2):
                    wide = []
                    for j in range(halves):
                        here = values[k][:, j * LANES : (j + 1) * LANES]
                        if chunk:
                            here = here + product[j, rows_of(k, f, count), :]
                        product[j, rows_of(k, f, count), :] = here
                        wide.append(here)
                    values[k] = jnp.concatenate(wide, axis=1)
                if chunk == chunks:
                    segment = add_segment(segment, values, f)
        if owners == [0]:
            pl.semaphore_wait(known, len(contacts))
        deliver(owners, product, segment)
    incoming[me_p] = outgoing[me_p]
    gathered[mine] = shares[me_p]

    aside = (lax.rem(me_p + 1, param_count), me_q)
    others = incoming.at[pl.ds(0, param_count - 1)]
    out_wait = pltpu.make_async_remote_copy(
        src_ref=others, dst_ref=others, send_sem=out_send, recv_sem=out_recv,
        device_id=aside, device_id_type=MESH,
    )
    others = gathered.at[pl.ds(0, qoi_count * param_count - 1)]
    share_wait = pltpu.make_async_remote_copy(
        src_ref=others, dst_ref=others, send_sem=share_send, recv_sem=share_recv,
        device_id=aside, device_id_type=MESH,
    )
    out_wait.wait_recv()
    total = incoming[0].astype(jnp.float32)
    for p in range(1, param_count):
        total = total + incoming[p].astype(jnp.float32)
    out_ref[...] = total.reshape(out_ref.shape)
    share_wait.wait_recv()
    final = gathered[0]
    for p in range(1, param_count * qoi_count):
        final = final + gathered[p]
    for k in range(2):
        rows = jnp.broadcast_to(final[k : k + 1], (freq_count, LANES))
        turned = pltpu.roll(rows, 0, 1, stride=GROUPS, stride_axis=0)
        seg_ref[0, k] = turned[:, :GROUPS]
    wait_line(0, chunks * freq_count + half_freqs, 0).wait_send()
    out_wait.wait_send()
    share_wait.wait_send()


def writer(spectrum_ref, response_ref, spectrum_hbm, response_hbm, sems):
    copies = [
        pltpu.make_async_copy(spectrum_ref, spectrum_hbm, sems.at[0]),
        pltpu.make_async_copy(response_ref, response_hbm, sems.at[1]),
    ]
    for copy in copies:
        copy.start()
    for copy in copies:
        copy.wait()


def local(samples, operator_rows, block_start, gauge_group):
    sample_local, param_local, steps_count = samples.shape
    freq_count, _, _, gauge_local = operator_rows.shape
    param_count, qoi_count = lax.axis_size("param"), lax.axis_size("qoi")
    sample_total = sample_local * qoi_count
    halves = gauge_local // LANES
    depth = 2 * param_local
    stripe = 2 * freq_count
    aligned = param_local // LANES * LANES
    tail = param_local - aligned
    assert sample_total == param_count and freq_count * GROUPS == LANES
    assert 2 * tail == LANES and freq_count % LOADS == 0 and steps_count % 2 == 0
    rows = operator_rows.reshape(freq_count, param_local, 2, halves, LANES)
    rows = rows.transpose(0, 1, 3, 2, 4).reshape(freq_count, depth * halves, LANES)
    dma = pltpu.SemaphoreType.DMA
    vmem = pl.BlockSpec(memory_space=pltpu.VMEM)
    hbm = pl.BlockSpec(memory_space=pltpu.HBM)
    shapes = (
        jax.ShapeDtypeStruct((1, 2, freq_count, gauge_local), jnp.float32),
        jax.ShapeDtypeStruct((1, 2, freq_count, GROUPS), jnp.float32),
    )
    found = pl.pallas_call(
        functools.partial(kernel, param_count, qoi_count),
        out_shape=shapes,
        in_specs=[pl.BlockSpec(memory_space=pltpu.SMEM), hbm, hbm, hbm],
        out_specs=(vmem, vmem),
        scratch_shapes=[
            pltpu.VMEM((1, gauge_local), jnp.int32),
            pltpu.VMEM((steps_count, sample_local, param_local), jnp.bfloat16),
            pltpu.VMEM((4 * freq_count * sample_local, steps_count // 2 * sample_local), jnp.bfloat16),
            pltpu.VMEM((freq_count, depth * halves, LANES), jnp.bfloat16),
            pltpu.VMEM((depth * halves, LANES), jnp.float32),
            pltpu.VMEM((freq_count, 2, aligned, gauge_local), jnp.bfloat16),
            pltpu.VMEM((freq_count // 2, 2, 2 * tail, gauge_local), jnp.bfloat16),
            pltpu.VMEM((freq_count, LANES, gauge_local), jnp.bfloat16),
            pltpu.VMEM(
                (qoi_count, aligned // LANES * freq_count + freq_count // 2, 2 * sample_local, LANES),
                jnp.bfloat16,
            ),
            pltpu.VMEM((halves, stripe * sample_local, LANES), jnp.float32),
            pltpu.VMEM((halves, stripe * (sample_total - sample_local), LANES), jnp.float32),
            pltpu.VMEM((sample_total, stripe, gauge_local), jnp.bfloat16),
            pltpu.VMEM((param_count, stripe, gauge_local), jnp.bfloat16),
            pltpu.VMEM((2 * sample_total, LANES), jnp.float32),
            pltpu.VMEM((sample_total, 2, LANES), jnp.float32),
            pltpu.VMEM((qoi_count * param_count, 2, LANES), jnp.float32),
            dma(()),
            dma((2,)),
            dma((LOADS,)),
            dma(()),
            dma((aligned // LANES + 1,)),
            dma(()),
            dma(()),
            dma(()),
            dma(()),
            pltpu.SemaphoreType.REGULAR,
        ],
        compiler_params=pltpu.CompilerParams(
            collective_id=0, has_side_effects=True, vmem_limit_bytes=53 * 2**20
        ),
    )(
        block_start,
        pltpu.with_memory_space_constraint(gauge_group.reshape(1, gauge_local), pltpu.HBM),
        samples.transpose(2, 0, 1),
        rows,
    )
    return pl.pallas_call(
        writer,
        out_shape=shapes,
        in_specs=[vmem, vmem],
        out_specs=(pl.BlockSpec(memory_space=pl.ANY), pl.BlockSpec(memory_space=pl.ANY)),
        scratch_shapes=[dma((2,))],
    )(*[pltpu.with_memory_space_constraint(array, pltpu.VMEM) for array in found])


def solution(mesh):
    return jax.shard_map(
        local,
        mesh=mesh,
        in_specs=(P("qoi", "param", None), P(None, "param", None, "qoi"), P(), P("qoi")),
        out_specs=(P("param", None, None, "qoi"), P("param", None, None, None)),
        check_vma=False,
    )
```

```python
import functools
import math

import jax
import jax.numpy as jnp
from jax import lax
from jax.experimental import pallas as pl
from jax.experimental.pallas import tpu as pltpu
from jax.sharding import PartitionSpec as P

GROUPS = 16
LANES = 128
LOADS = 2
MESH = pl.DeviceIdType.MESH
NT_DIMS = (((1,), (1,)), ((), ()))


def build_table(start, freq_count, steps_count, count, repeat, table):
    shape = (freq_count, count * repeat)
    steps = lax.broadcasted_iota(jnp.int32, shape, 1) // repeat
    freqs = lax.broadcasted_iota(jnp.int32, shape, 0) + start
    turns = (steps * freqs).astype(jnp.float32)
    whole = jnp.floor((turns + 0.5) * (1.0 / steps_count))
    phases = (turns - whole * steps_count) * (2.0 * math.pi / steps_count)
    scale = 1.0 / math.sqrt(steps_count)
    waves = [jnp.cos(phases) * scale, jnp.sin(phases) * -scale]
    highs = [wave.astype(jnp.bfloat16).astype(jnp.float32) for wave in waves]
    lows = [wave - high for wave, high in zip(waves, highs)]
    full = (repeat, count * repeat)
    keep = lax.broadcasted_iota(jnp.int32, full, 1) % repeat == lax.broadcasted_iota(
        jnp.int32, full, 0
    )
    for level, pair in enumerate((highs, lows)):
        for f in range(freq_count):
            rows = jnp.concatenate(
                [jnp.where(keep, jnp.broadcast_to(wave[f : f + 1], full), 0.0) for wave in pair],
                axis=0,
            )
            first = (level * freq_count + f) * 2 * repeat
            table[pl.ds(first, 2 * repeat), :] = rows.astype(jnp.bfloat16)


def kernel(
    param_count, qoi_count, start_ref, group_hbm, samples_hbm, rows_hbm,
    out_ref, seg_ref,
    group_ref, samples, table, weights, loose, dense, dense_tail, grouped, grouped_tail, hot, line, near, far, outgoing, incoming, joined, shares, gathered,
    group_sem, samples_sem, weights_sem, line_send, line_recv, out_send, out_recv, share_send, share_recv, known,
):
    steps_count, sample_local, param_local = samples.shape
    freq_count = weights.shape[0]
    gauge_local = group_ref.shape[1]
    halves = gauge_local // LANES
    aligned = param_local // LANES * LANES
    tail = param_local - aligned
    chunks = aligned // LANES
    pair_rows = 2 * sample_local
    half_freqs = freq_count // 2
    half_steps = steps_count // 2
    stripe = 2 * freq_count
    inner = 2 ** (int(math.log2(param_count)) // 2)
    me_p = lax.axis_index("param")
    me_q = lax.axis_index("qoi")
    base = me_p // inner * inner

    contacts = []
    for turn in range(1, param_count // inner):
        contacts.append((lax.rem(me_p + turn * inner, param_count), me_q))
    for other in reversed(range(qoi_count)):
        for turn in range(inner):
            if other or turn:
                contacts.append(
                    (base + lax.rem(me_p + turn, inner), lax.rem(me_q + other, qoi_count))
                )
    barrier = pltpu.get_barrier_semaphore()
    group_copy = pltpu.make_async_copy(group_hbm, group_ref, group_sem)
    group_copy.start()
    lanes = [pl.ds(0, aligned), pl.ds(aligned, tail)]
    sample_copies = [
        pltpu.make_async_copy(samples_hbm.at[:, :, lane], samples.at[:, :, lane], samples_sem.at[part])
        for part, lane in enumerate(lanes)
    ]
    for copy in sample_copies:
        copy.start()
    for contact in contacts:
        pl.semaphore_signal(barrier, inc=1, device_id=contact, device_id_type=MESH)
    per_load = freq_count // LOADS
    loads = [pl.ds(load * per_load, per_load) for load in range(LOADS)]
    weight_copies = [
        pltpu.make_async_copy(rows_hbm.at[load], weights.at[load], weights_sem.at[index])
        for index, load in enumerate(loads)
    ]

    start = start_ref[0]
    build_table(start, freq_count, steps_count, half_steps, sample_local, table)
    for copy in weight_copies:
        copy.start()

    sample_copies[0].wait()

    def send_line(first, count, index):
        picked = pl.ds(first, count)
        for offset in range(1, qoi_count):
            pltpu.make_async_remote_copy(
                src_ref=line.at[me_q, picked],
                dst_ref=line.at[me_q, picked],
                send_sem=line_send,
                recv_sem=line_recv.at[index],
                device_id=(me_p, lax.rem(me_q + offset, qoi_count)),
                device_id_type=MESH,
            ).start()

    def wait_line(first, count, index):
        others = line.at[pl.ds(0, qoi_count - 1), pl.ds(first, count)]
        return pltpu.make_async_remote_copy(
            src_ref=others,
            dst_ref=others,
            send_sem=line_send,
            recv_sem=line_recv.at[index],
            device_id=(me_p, lax.rem(me_q + 1, qoi_count)),
            device_id_type=MESH,
        )

    turns = table[...]
    half = freq_count * pair_rows
    sides, ends = [], []
    for part in range(2):
        block = samples[pl.ds(part * half_steps, half_steps), :, pl.ds(0, aligned)]
        block = block.reshape(half_steps * sample_local, aligned)
        both = jnp.dot(turns, block, preferred_element_type=jnp.float32)
        sides.append(both[:half] + both[half:])
    odd = lax.rem(start + lax.broadcasted_iota(jnp.int32, (half, LANES), 0) // pair_rows, 2)
    sign = 1.0 - 2.0 * odd.astype(jnp.float32)
    pl.semaphore_wait(barrier, len(contacts))
    for chunk in range(chunks):
        columns = slice(chunk * LANES, (chunk + 1) * LANES)
        spectrum = sides[0][:, columns] + sign * sides[1][:, columns]
        line[me_q, chunk * freq_count : (chunk + 1) * freq_count] = spectrum.astype(
            jnp.bfloat16
        ).reshape(freq_count, pair_rows, LANES)
        send_line(chunk * freq_count, freq_count, chunk)
    for contact in contacts:
        pl.semaphore_signal(known, inc=1, device_id=contact, device_id_type=MESH)
    sample_copies[1].wait()
    for part in range(2):
        block = samples[pl.ds(part * half_steps, half_steps), :, pl.ds(aligned, tail)]
        ends.append(block.reshape(half_steps * sample_local, tail))
    both = jnp.dot(turns, jnp.concatenate(ends, axis=1), preferred_element_type=jnp.float32)
    both = both[:half] + both[half:]
    both = both + sign * pltpu.roll(both, tail, 1)
    middle = half // 2
    lane = lax.broadcasted_iota(jnp.int32, (middle, LANES), 1)
    packed = jnp.where(lane < tail, both[:middle], both[middle:] * sign[middle:])
    line[me_q, chunks * freq_count :] = packed.astype(jnp.bfloat16).reshape(
        half_freqs, pair_rows, LANES
    )
    send_line(chunks * freq_count, half_freqs, chunks)

    group_copy.wait()
    slots = lax.broadcasted_iota(jnp.int32, (LANES, gauge_local), 0)
    for f in range(freq_count):
        place = (freq_count - f) % freq_count * GROUPS
        hot[f] = (slots == group_ref[...] + place).astype(jnp.float32).astype(jnp.bfloat16)

    def group_sums(right, f):
        sums = lax.dot_general(right, hot[f], NT_DIMS, preferred_element_type=jnp.float32)
        return sums.astype(jnp.bfloat16)

    for f in range(freq_count):
        if f % per_load == 0:
            weight_copies[f // per_load].wait()
        loose[...] = weights[f].astype(jnp.float32)
        for j in range(halves):
            columns = pl.ds(j * LANES, LANES)
            for part in range(2):
                piece = loose[
                    pl.ds(2 * j + part, param_local, stride=2 * halves), :
                ].astype(jnp.bfloat16)
                dense[f, part, :, columns] = piece[:aligned]
                dense_tail[f % half_freqs, part, pl.ds(f // half_freqs * tail, tail), columns] = (
                    piece[aligned:]
                )
        for part in range(2):
            ending = pl.ds(f // half_freqs * tail, tail)
            grouped_tail[f % half_freqs, part, ending] = group_sums(
                dense_tail[f % half_freqs, part, ending], f
            )
            sums = group_sums(dense[f, part], f)
            for chunk in range(chunks):
                grouped[chunk, part, f] = sums[chunk * LANES : (chunk + 1) * LANES]

    mine = me_q * param_count + me_p
    ratio = math.sqrt(GROUPS / (gauge_local * qoi_count))

    def combine(sides):
        real, imag = sides
        results = [[], []]
        for index in range(real.shape[0] // pair_rows):
            low, mid, high = [index * pair_rows + step * sample_local for step in range(3)]
            results[0].append(real[low:mid] - imag[mid:high])
            results[1].append(imag[low:mid] + real[mid:high])
        return [jnp.concatenate(result, axis=0) for result in results]

    def multiply(owners, f, chunk):
        if chunk < chunks:
            left = jnp.concatenate([line[q, chunk * freq_count + f] for q in owners], axis=0)
            right = [dense[f, part, chunk * LANES : (chunk + 1) * LANES, :] for part in range(2)]
        else:
            left = jnp.concatenate(
                [line[q, chunks * freq_count + f % half_freqs] for q in owners], axis=0
            )
            lane = lax.broadcasted_iota(jnp.int32, left.shape, 1)
            left = jnp.where((lane >= tail) == (f >= half_freqs), left.astype(jnp.float32), 0.0)
            left = left.astype(jnp.bfloat16)
            right = [dense_tail[f % half_freqs, part] for part in range(2)]
        return combine(
            [jnp.dot(left, side, preferred_element_type=jnp.float32) for side in right]
        )

    def group_products(owners, chunk):
        tiles = freq_count if chunk < chunks else half_freqs
        left = jnp.concatenate(
            [
                jnp.concatenate([line[q, chunk * freq_count + tile] for tile in range(tiles)], axis=1)
                for q in owners
            ],
            axis=0,
        )
        right = grouped.at[chunk] if chunk < chunks else grouped_tail
        results = []
        for part in range(2):
            if chunk < chunks:
                side = right[part]
            else:
                side = jnp.stack([right[tile, part] for tile in range(tiles)], axis=0)
            side = side.reshape(tiles * LANES, LANES)
            results.append(jnp.dot(left, side, preferred_element_type=jnp.float32))
        return results

    def rows_of(k, f, count):
        return pl.ds((k * freq_count + f) * count, count)

    def deliver_shares(owners, segment):
        count = len(owners) * sample_local
        joined[pl.ds(0, 2 * count), :] = segment * ratio
        for index, q in enumerate(owners):
            for i in range(sample_local):
                shares[q * sample_local + i] = joined[
                    pl.ds(index * sample_local + i, 2, stride=count), :
                ]
        for away in reversed(range(qoi_count)):
            for q in owners:
                for i in range(sample_local):
                    target = q * sample_local + i
                    copy = pltpu.make_async_remote_copy(
                        src_ref=shares.at[target],
                        dst_ref=gathered.at[mine],
                        send_sem=share_send,
                        recv_sem=share_recv,
                        device_id=(target, lax.rem(me_q + away, qoi_count)),
                        device_id_type=MESH,
                    )
                    if away:
                        copy.start()
                    else:
                        pl.when(target != me_p)(copy.start)

    def deliver_blocks(owners, product):
        count = len(owners) * sample_local
        for index, q in enumerate(owners):
            for i in range(sample_local):
                for j in range(halves):
                    outgoing[q * sample_local + i, :, j * LANES : (j + 1) * LANES] = product[
                        j, pl.ds(index * sample_local + i, stripe, stride=count), :
                    ].astype(jnp.bfloat16)
        for q in owners:
            for i in range(sample_local):
                target = q * sample_local + i
                copy = pltpu.make_async_remote_copy(
                    src_ref=outgoing.at[target],
                    dst_ref=incoming.at[me_p],
                    send_sem=out_send,
                    recv_sem=out_recv,
                    device_id=(target, me_q),
                    device_id_type=MESH,
                )
                pl.when(target != me_p)(copy.start)

    for owners, product in (([0], near), (list(range(1, qoi_count)), far)):
        count = len(owners) * sample_local
        totals = None
        for chunk in range(chunks + 1):
            rows = freq_count if chunk < chunks else half_freqs
            line_wait = wait_line(chunk * freq_count, rows, chunk)
            pl.when(me_q != 0 if owners == [0] else me_q == 0)(line_wait.wait_recv)
            sums = group_products(owners, chunk)
            totals = sums if totals is None else [a + b for a, b in zip(totals, sums)]
            if chunk == chunks:
                if owners == [0]:
                    pl.semaphore_wait(known, len(contacts))
                deliver_shares(owners, jnp.concatenate(combine(totals), axis=0))
            for f in range(freq_count):
                for k, value in enumerate(multiply(owners, f, chunk)):
                    for j in range(halves):
                        here = value[:, j * LANES : (j + 1) * LANES]
                        if chunk:
                            here = here + product[j, rows_of(k, f, count), :]
                        product[j, rows_of(k, f, count), :] = here
        deliver_blocks(owners, product)
    incoming[me_p] = outgoing[me_p]
    gathered[mine] = shares[me_p]

    aside = (lax.rem(me_p + 1, param_count), me_q)
    others = incoming.at[pl.ds(0, param_count - 1)]
    out_wait = pltpu.make_async_remote_copy(
        src_ref=others, dst_ref=others, send_sem=out_send, recv_sem=out_recv,
        device_id=aside, device_id_type=MESH,
    )
    others = gathered.at[pl.ds(0, qoi_count * param_count - 1)]
    share_wait = pltpu.make_async_remote_copy(
        src_ref=others, dst_ref=others, send_sem=share_send, recv_sem=share_recv,
        device_id=aside, device_id_type=MESH,
    )
    out_wait.wait_recv()
    total = incoming[0].astype(jnp.float32)
    for p in range(1, param_count):
        total = total + incoming[p].astype(jnp.float32)
    out_ref[...] = total.reshape(out_ref.shape)
    share_wait.wait_recv()
    final = gathered[0]
    for p in range(1, param_count * qoi_count):
        final = final + gathered[p]
    for k in range(2):
        rows = jnp.broadcast_to(final[k : k + 1], (freq_count, LANES))
        turned = pltpu.roll(rows, 0, 1, stride=GROUPS, stride_axis=0)
        seg_ref[0, k] = turned[:, :GROUPS]
    wait_line(0, chunks * freq_count + half_freqs, 0).wait_send()
    out_wait.wait_send()
    share_wait.wait_send()


def writer(spectrum_ref, response_ref, spectrum_hbm, response_hbm, sems):
    copies = [
        pltpu.make_async_copy(spectrum_ref, spectrum_hbm, sems.at[0]),
        pltpu.make_async_copy(response_ref, response_hbm, sems.at[1]),
    ]
    for copy in copies:
        copy.start()
    for copy in copies:
        copy.wait()


def local(samples, operator_rows, block_start, gauge_group):
    sample_local, param_local, steps_count = samples.shape
    freq_count, _, _, gauge_local = operator_rows.shape
    param_count, qoi_count = lax.axis_size("param"), lax.axis_size("qoi")
    sample_total = sample_local * qoi_count
    halves = gauge_local // LANES
    depth = 2 * param_local
    stripe = 2 * freq_count
    aligned = param_local // LANES * LANES
    tail = param_local - aligned
    assert sample_total == param_count and freq_count * GROUPS == LANES
    assert 2 * tail == LANES and freq_count % LOADS == 0 and steps_count % 2 == 0
    rows = operator_rows.reshape(freq_count, param_local, 2, halves, LANES)
    rows = rows.transpose(0, 1, 3, 2, 4).reshape(freq_count, depth * halves, LANES)
    dma = pltpu.SemaphoreType.DMA
    vmem = pl.BlockSpec(memory_space=pltpu.VMEM)
    hbm = pl.BlockSpec(memory_space=pltpu.HBM)
    shapes = (
        jax.ShapeDtypeStruct((1, 2, freq_count, gauge_local), jnp.float32),
        jax.ShapeDtypeStruct((1, 2, freq_count, GROUPS), jnp.float32),
    )
    found = pl.pallas_call(
        functools.partial(kernel, param_count, qoi_count),
        out_shape=shapes,
        in_specs=[pl.BlockSpec(memory_space=pltpu.SMEM), hbm, hbm, hbm],
        out_specs=(vmem, vmem),
        scratch_shapes=[
            pltpu.VMEM((1, gauge_local), jnp.int32),
            pltpu.VMEM((steps_count, sample_local, param_local), jnp.bfloat16),
            pltpu.VMEM((4 * freq_count * sample_local, steps_count // 2 * sample_local), jnp.bfloat16),
            pltpu.VMEM((freq_count, depth * halves, LANES), jnp.bfloat16),
            pltpu.VMEM((depth * halves, LANES), jnp.float32),
            pltpu.VMEM((freq_count, 2, aligned, gauge_local), jnp.bfloat16),
            pltpu.VMEM((freq_count // 2, 2, 2 * tail, gauge_local), jnp.bfloat16),
            pltpu.VMEM((aligned // LANES, 2, freq_count, LANES, LANES), jnp.bfloat16),
            pltpu.VMEM((freq_count // 2, 2, 2 * tail, LANES), jnp.bfloat16),
            pltpu.VMEM((freq_count, LANES, gauge_local), jnp.bfloat16),
            pltpu.VMEM(
                (qoi_count, aligned // LANES * freq_count + freq_count // 2, 2 * sample_local, LANES),
                jnp.bfloat16,
            ),
            pltpu.VMEM((halves, stripe * sample_local, LANES), jnp.float32),
            pltpu.VMEM((halves, stripe * (sample_total - sample_local), LANES), jnp.float32),
            pltpu.VMEM((sample_total, stripe, gauge_local), jnp.bfloat16),
            pltpu.VMEM((param_count, stripe, gauge_local), jnp.bfloat16),
            pltpu.VMEM((2 * sample_total, LANES), jnp.float32),
            pltpu.VMEM((sample_total, 2, LANES), jnp.float32),
            pltpu.VMEM((qoi_count * param_count, 2, LANES), jnp.float32),
            dma(()),
            dma((2,)),
            dma((LOADS,)),
            dma(()),
            dma((aligned // LANES + 1,)),
            dma(()),
            dma(()),
            dma(()),
            dma(()),
            pltpu.SemaphoreType.REGULAR,
        ],
        compiler_params=pltpu.CompilerParams(
            collective_id=0, has_side_effects=True, vmem_limit_bytes=53 * 2**20
        ),
    )(
        block_start,
        pltpu.with_memory_space_constraint(gauge_group.reshape(1, gauge_local), pltpu.HBM),
        samples.transpose(2, 0, 1),
        rows,
    )
    return pl.pallas_call(
        writer,
        out_shape=shapes,
        in_specs=[vmem, vmem],
        out_specs=(pl.BlockSpec(memory_space=pl.ANY), pl.BlockSpec(memory_space=pl.ANY)),
        scratch_shapes=[dma((2,))],
    )(*[pltpu.with_memory_space_constraint(array, pltpu.VMEM) for array in found])


def solution(mesh):
    return jax.shard_map(
        local,
        mesh=mesh,
        in_specs=(P("qoi", "param", None), P(None, "param", None, "qoi"), P(), P("qoi")),
        out_specs=(P("param", None, None, "qoi"), P("param", None, None, None)),
        check_vma=False,
    )
```

```python
import functools
import math

import jax
import jax.numpy as jnp
from jax import lax
from jax.experimental import pallas as pl
from jax.experimental.pallas import tpu as pltpu
from jax.sharding import PartitionSpec as P

GROUPS = 16
LANES = 128
LOADS = 2
MESH = pl.DeviceIdType.MESH
NT_DIMS = (((1,), (1,)), ((), ()))


def build_table(start, freq_count, steps_count, count, repeat, table):
    shape = (freq_count, count * repeat)
    steps = lax.broadcasted_iota(jnp.int32, shape, 1) // repeat
    freqs = lax.broadcasted_iota(jnp.int32, shape, 0) + start
    turns = (steps * freqs).astype(jnp.float32)
    whole = jnp.floor((turns + 0.5) * (1.0 / steps_count))
    phases = (turns - whole * steps_count) * (2.0 * math.pi / steps_count)
    scale = 1.0 / math.sqrt(steps_count)
    waves = [jnp.cos(phases) * scale, jnp.sin(phases) * -scale]
    highs = [wave.astype(jnp.bfloat16).astype(jnp.float32) for wave in waves]
    lows = [wave - high for wave, high in zip(waves, highs)]
    full = (repeat, count * repeat)
    keep = lax.broadcasted_iota(jnp.int32, full, 1) % repeat == lax.broadcasted_iota(
        jnp.int32, full, 0
    )
    for level, pair in enumerate((highs, lows)):
        for f in range(freq_count):
            rows = jnp.concatenate(
                [jnp.where(keep, jnp.broadcast_to(wave[f : f + 1], full), 0.0) for wave in pair],
                axis=0,
            )
            first = (level * freq_count + f) * 2 * repeat
            table[pl.ds(first, 2 * repeat), :] = rows.astype(jnp.bfloat16)


def kernel(
    param_count, qoi_count, start_ref, group_hbm, samples_hbm, rows_hbm,
    out_ref, seg_ref,
    group_ref, samples, table, weights, loose, dense, dense_tail, grouped, grouped_tail, hot, line, near, far, outgoing, incoming, joined, shares, gathered,
    group_sem, samples_sem, weights_sem, line_send, line_recv, out_send, out_recv, share_send, share_recv, known,
):
    steps_count, sample_local, param_local = samples.shape
    freq_count = weights.shape[0]
    gauge_local = group_ref.shape[1]
    halves = gauge_local // LANES
    aligned = param_local // LANES * LANES
    tail = param_local - aligned
    chunks = aligned // LANES
    pair_rows = 2 * sample_local
    half_freqs = freq_count // 2
    half_steps = steps_count // 2
    stripe = 2 * freq_count
    inner = 2 ** (int(math.log2(param_count)) // 2)
    me_p = lax.axis_index("param")
    me_q = lax.axis_index("qoi")
    base = me_p // inner * inner

    contacts = []
    for turn in range(1, param_count // inner):
        contacts.append((lax.rem(me_p + turn * inner, param_count), me_q))
    for other in reversed(range(qoi_count)):
        for turn in range(inner):
            if other or turn:
                contacts.append(
                    (base + lax.rem(me_p + turn, inner), lax.rem(me_q + other, qoi_count))
                )
    barrier = pltpu.get_barrier_semaphore()
    group_copy = pltpu.make_async_copy(group_hbm, group_ref, group_sem)
    group_copy.start()
    lanes = [pl.ds(0, aligned), pl.ds(aligned, tail)]
    sample_copies = [
        pltpu.make_async_copy(samples_hbm.at[:, :, lane], samples.at[:, :, lane], samples_sem.at[part])
        for part, lane in enumerate(lanes)
    ]
    for copy in sample_copies:
        copy.start()
    for contact in contacts:
        pl.semaphore_signal(barrier, inc=1, device_id=contact, device_id_type=MESH)
    per_load = freq_count // LOADS
    loads = [pl.ds(load * per_load, per_load) for load in range(LOADS)]
    weight_copies = [
        pltpu.make_async_copy(rows_hbm.at[load], weights.at[load], weights_sem.at[index])
        for index, load in enumerate(loads)
    ]

    start = start_ref[0]
    build_table(start, freq_count, steps_count, half_steps, sample_local, table)
    for copy in weight_copies:
        copy.start()

    sample_copies[0].wait()

    def send_line(first, count, index):
        picked = pl.ds(first, count)
        for offset in range(1, qoi_count):
            pltpu.make_async_remote_copy(
                src_ref=line.at[me_q, picked],
                dst_ref=line.at[me_q, picked],
                send_sem=line_send,
                recv_sem=line_recv.at[index],
                device_id=(me_p, lax.rem(me_q + offset, qoi_count)),
                device_id_type=MESH,
            ).start()

    def wait_line(first, count, index):
        others = line.at[pl.ds(0, qoi_count - 1), pl.ds(first, count)]
        return pltpu.make_async_remote_copy(
            src_ref=others,
            dst_ref=others,
            send_sem=line_send,
            recv_sem=line_recv.at[index],
            device_id=(me_p, lax.rem(me_q + 1, qoi_count)),
            device_id_type=MESH,
        )

    turns = table[...]
    half = freq_count * pair_rows
    sides, ends = [], []
    for part in range(2):
        block = samples[pl.ds(part * half_steps, half_steps), :, pl.ds(0, aligned)]
        block = block.reshape(half_steps * sample_local, aligned)
        both = jnp.dot(turns, block, preferred_element_type=jnp.float32)
        sides.append(both[:half] + both[half:])
    odd = lax.rem(start + lax.broadcasted_iota(jnp.int32, (half, LANES), 0) // pair_rows, 2)
    sign = 1.0 - 2.0 * odd.astype(jnp.float32)
    pl.semaphore_wait(barrier, len(contacts))
    for chunk in range(chunks):
        columns = slice(chunk * LANES, (chunk + 1) * LANES)
        spectrum = sides[0][:, columns] + sign * sides[1][:, columns]
        line[me_q, chunk * freq_count : (chunk + 1) * freq_count] = spectrum.astype(
            jnp.bfloat16
        ).reshape(freq_count, pair_rows, LANES)
        send_line(chunk * freq_count, freq_count, chunk)
    for contact in contacts:
        pl.semaphore_signal(known, inc=1, device_id=contact, device_id_type=MESH)
    sample_copies[1].wait()
    for part in range(2):
        block = samples[pl.ds(part * half_steps, half_steps), :, pl.ds(aligned, tail)]
        ends.append(block.reshape(half_steps * sample_local, tail))
    both = jnp.dot(turns, jnp.concatenate(ends, axis=1), preferred_element_type=jnp.float32)
    both = both[:half] + both[half:]
    both = both + sign * pltpu.roll(both, tail, 1)
    middle = half // 2
    lane = lax.broadcasted_iota(jnp.int32, (middle, LANES), 1)
    packed = jnp.where(lane < tail, both[:middle], both[middle:] * sign[middle:])
    line[me_q, chunks * freq_count :] = packed.astype(jnp.bfloat16).reshape(
        half_freqs, pair_rows, LANES
    )
    send_line(chunks * freq_count, half_freqs, chunks)

    group_copy.wait()
    slots = lax.broadcasted_iota(jnp.int32, (LANES, gauge_local), 0)
    for f in range(freq_count):
        place = (freq_count - f) % freq_count * GROUPS
        hot[f] = (slots == group_ref[...] + place).astype(jnp.float32).astype(jnp.bfloat16)

    for f in range(freq_count):
        if f % per_load == 0:
            weight_copies[f // per_load].wait()
        loose[...] = weights[f].astype(jnp.float32)
        for part in range(2):
            piece = jnp.concatenate(
                [
                    loose[pl.ds(2 * j + part, param_local, stride=2 * halves), :]
                    for j in range(halves)
                ],
                axis=1,
            ).astype(jnp.bfloat16)
            dense[f, part] = piece[:aligned]
            dense_tail[f % half_freqs, part, pl.ds(f // half_freqs * tail, tail)] = piece[aligned:]

    mine = me_q * param_count + me_p
    ratio = math.sqrt(GROUPS / (gauge_local * qoi_count))

    def combine(sides):
        real, imag = sides
        results = [[], []]
        for index in range(real.shape[0] // pair_rows):
            low, mid, high = [index * pair_rows + step * sample_local for step in range(3)]
            results[0].append(real[low:mid] - imag[mid:high])
            results[1].append(imag[low:mid] + real[mid:high])
        return [jnp.concatenate(result, axis=0) for result in results]

    def multiply(owners, f, chunk):
        if chunk < chunks:
            left = jnp.concatenate([line[q, chunk * freq_count + f] for q in owners], axis=0)
            right = [dense[f, part, chunk * LANES : (chunk + 1) * LANES, :] for part in range(2)]
        else:
            left = jnp.concatenate(
                [line[q, chunks * freq_count + f % half_freqs] for q in owners], axis=0
            )
            lane = lax.broadcasted_iota(jnp.int32, left.shape, 1)
            left = jnp.where((lane >= tail) == (f >= half_freqs), left.astype(jnp.float32), 0.0)
            left = left.astype(jnp.bfloat16)
            right = [dense_tail[f % half_freqs, part] for part in range(2)]
        return combine(
            [jnp.dot(left, side, preferred_element_type=jnp.float32) for side in right]
        )

    def build_grouped():
        for f in range(freq_count):
            ending = pl.ds(f // half_freqs * tail, tail)
            rows = []
            for part in range(2):
                rows += [dense[f, part], dense_tail[f % half_freqs, part, ending]]
            sums = lax.dot_general(
                jnp.concatenate(rows, axis=0), hot[f], NT_DIMS, preferred_element_type=jnp.float32
            ).astype(jnp.bfloat16)
            for part in range(2):
                first = part * param_local
                for chunk in range(chunks):
                    row = first + chunk * LANES
                    grouped[chunk, part, f] = sums[row : row + LANES]
                grouped_tail[f % half_freqs, part, ending] = sums[
                    first + aligned : first + param_local
                ]

    def group_products(owners, chunk):
        tiles = freq_count if chunk < chunks else half_freqs
        left = jnp.concatenate(
            [
                jnp.concatenate([line[q, chunk * freq_count + tile] for tile in range(tiles)], axis=1)
                for q in owners
            ],
            axis=0,
        )
        right = grouped.at[chunk] if chunk < chunks else grouped_tail
        results = []
        for part in range(2):
            if chunk < chunks:
                side = right[part]
            else:
                side = jnp.stack([right[tile, part] for tile in range(tiles)], axis=0)
            side = side.reshape(tiles * LANES, LANES)
            results.append(jnp.dot(left, side, preferred_element_type=jnp.float32))
        return results

    def rows_of(k, f, count):
        return pl.ds((k * freq_count + f) * count, count)

    def deliver_shares(owners, segment):
        count = len(owners) * sample_local
        joined[pl.ds(0, 2 * count), :] = segment * ratio
        for index, q in enumerate(owners):
            for i in range(sample_local):
                shares[q * sample_local + i] = joined[
                    pl.ds(index * sample_local + i, 2, stride=count), :
                ]
        for away in reversed(range(qoi_count)):
            for q in owners:
                for i in range(sample_local):
                    target = q * sample_local + i
                    copy = pltpu.make_async_remote_copy(
                        src_ref=shares.at[target],
                        dst_ref=gathered.at[mine],
                        send_sem=share_send,
                        recv_sem=share_recv,
                        device_id=(target, lax.rem(me_q + away, qoi_count)),
                        device_id_type=MESH,
                    )
                    if away:
                        copy.start()
                    else:
                        pl.when(target != me_p)(copy.start)

    def deliver_blocks(owners, product):
        count = len(owners) * sample_local
        for index, q in enumerate(owners):
            for i in range(sample_local):
                for j in range(halves):
                    outgoing[q * sample_local + i, :, j * LANES : (j + 1) * LANES] = product[
                        j, pl.ds(index * sample_local + i, stripe, stride=count), :
                    ].astype(jnp.bfloat16)
        for q in owners:
            for i in range(sample_local):
                target = q * sample_local + i
                copy = pltpu.make_async_remote_copy(
                    src_ref=outgoing.at[target],
                    dst_ref=incoming.at[me_p],
                    send_sem=out_send,
                    recv_sem=out_recv,
                    device_id=(target, me_q),
                    device_id_type=MESH,
                )
                pl.when(target != me_p)(copy.start)

    def add_products(owners, product, chunk):
        count = len(owners) * sample_local
        for f in range(freq_count):
            for k, value in enumerate(multiply(owners, f, chunk)):
                for j in range(halves):
                    here = value[:, j * LANES : (j + 1) * LANES]
                    if chunk:
                        here = here + product[j, rows_of(k, f, count), :]
                    product[j, rows_of(k, f, count), :] = here

    def await_known():
        pl.semaphore_wait(known, len(contacts))

    def wait_chunk(chunk):
        rows = freq_count if chunk < chunks else half_freqs
        wait_line(chunk * freq_count, rows, chunk).wait_recv()

    def send_shares(owners, before_chunk, before_sending, after_chunk):
        totals = None
        for chunk in range(chunks + 1):
            before_chunk(chunk)
            sums = group_products(owners, chunk)
            totals = sums if totals is None else [a + b for a, b in zip(totals, sums)]
            if chunk == chunks:
                before_sending()
                deliver_shares(owners, jnp.concatenate(combine(totals), axis=0))
            after_chunk(chunk)

    def nothing(*_):
        pass

    def receive(owners, product, before_sending):
        def early(chunk):
            if chunk < chunks - 1:
                add_products(owners, product, chunk)

        send_shares(owners, wait_chunk, before_sending, early)
        for chunk in range(max(chunks - 1, 0), chunks + 1):
            add_products(owners, product, chunk)
        deliver_blocks(owners, product)

    def serve(owners, product, before_sending, after_blocks):
        for chunk in range(chunks + 1):
            add_products(owners, product, chunk)
        before_sending()
        deliver_blocks(owners, product)
        after_blocks()
        send_shares(owners, nothing, nothing, nothing)

    rest = list(range(1, qoi_count))

    @pl.when(me_q == 0)
    def _():
        serve([0], near, await_known, build_grouped)
        receive(rest, far, nothing)

    @pl.when(me_q != 0)
    def _():
        build_grouped()
        receive([0], near, await_known)
        serve(rest, far, nothing, nothing)

    incoming[me_p] = outgoing[me_p]
    gathered[mine] = shares[me_p]

    aside = (lax.rem(me_p + 1, param_count), me_q)
    others = incoming.at[pl.ds(0, param_count - 1)]
    out_wait = pltpu.make_async_remote_copy(
        src_ref=others, dst_ref=others, send_sem=out_send, recv_sem=out_recv,
        device_id=aside, device_id_type=MESH,
    )
    others = gathered.at[pl.ds(0, qoi_count * param_count - 1)]
    share_wait = pltpu.make_async_remote_copy(
        src_ref=others, dst_ref=others, send_sem=share_send, recv_sem=share_recv,
        device_id=aside, device_id_type=MESH,
    )
    out_wait.wait_recv()
    total = incoming[0].astype(jnp.float32)
    for p in range(1, param_count):
        total = total + incoming[p].astype(jnp.float32)
    out_ref[...] = total.reshape(out_ref.shape)
    share_wait.wait_recv()
    final = gathered[0]
    for p in range(1, param_count * qoi_count):
        final = final + gathered[p]
    for k in range(2):
        rows = jnp.broadcast_to(final[k : k + 1], (freq_count, LANES))
        turned = pltpu.roll(rows, 0, 1, stride=GROUPS, stride_axis=0)
        seg_ref[0, k] = turned[:, :GROUPS]
    wait_line(0, chunks * freq_count + half_freqs, 0).wait_send()
    out_wait.wait_send()
    share_wait.wait_send()


def writer(spectrum_ref, response_ref, spectrum_hbm, response_hbm, sems):
    copies = [
        pltpu.make_async_copy(spectrum_ref, spectrum_hbm, sems.at[0]),
        pltpu.make_async_copy(response_ref, response_hbm, sems.at[1]),
    ]
    for copy in copies:
        copy.start()
    for copy in copies:
        copy.wait()


def local(samples, operator_rows, block_start, gauge_group):
    sample_local, param_local, steps_count = samples.shape
    freq_count, _, _, gauge_local = operator_rows.shape
    param_count, qoi_count = lax.axis_size("param"), lax.axis_size("qoi")
    sample_total = sample_local * qoi_count
    halves = gauge_local // LANES
    depth = 2 * param_local
    stripe = 2 * freq_count
    aligned = param_local // LANES * LANES
    tail = param_local - aligned
    assert sample_total == param_count and freq_count * GROUPS == LANES
    assert 2 * tail == LANES and freq_count % LOADS == 0 and steps_count % 2 == 0
    rows = operator_rows.reshape(freq_count, param_local, 2, halves, LANES)
    rows = rows.transpose(0, 1, 3, 2, 4).reshape(freq_count, depth * halves, LANES)
    dma = pltpu.SemaphoreType.DMA
    vmem = pl.BlockSpec(memory_space=pltpu.VMEM)
    hbm = pl.BlockSpec(memory_space=pltpu.HBM)
    shapes = (
        jax.ShapeDtypeStruct((1, 2, freq_count, gauge_local), jnp.float32),
        jax.ShapeDtypeStruct((1, 2, freq_count, GROUPS), jnp.float32),
    )
    found = pl.pallas_call(
        functools.partial(kernel, param_count, qoi_count),
        out_shape=shapes,
        in_specs=[pl.BlockSpec(memory_space=pltpu.SMEM), hbm, hbm, hbm],
        out_specs=(vmem, vmem),
        scratch_shapes=[
            pltpu.VMEM((1, gauge_local), jnp.int32),
            pltpu.VMEM((steps_count, sample_local, param_local), jnp.bfloat16),
            pltpu.VMEM((4 * freq_count * sample_local, steps_count // 2 * sample_local), jnp.bfloat16),
            pltpu.VMEM((freq_count, depth * halves, LANES), jnp.bfloat16),
            pltpu.VMEM((depth * halves, LANES), jnp.float32),
            pltpu.VMEM((freq_count, 2, aligned, gauge_local), jnp.bfloat16),
            pltpu.VMEM((freq_count // 2, 2, 2 * tail, gauge_local), jnp.bfloat16),
            pltpu.VMEM((aligned // LANES, 2, freq_count, LANES, LANES), jnp.bfloat16),
            pltpu.VMEM((freq_count // 2, 2, 2 * tail, LANES), jnp.bfloat16),
            pltpu.VMEM((freq_count, LANES, gauge_local), jnp.bfloat16),
            pltpu.VMEM(
                (qoi_count, aligned // LANES * freq_count + freq_count // 2, 2 * sample_local, LANES),
                jnp.bfloat16,
            ),
            pltpu.VMEM((halves, stripe * sample_local, LANES), jnp.float32),
            pltpu.VMEM((halves, stripe * (sample_total - sample_local), LANES), jnp.float32),
            pltpu.VMEM((sample_total, stripe, gauge_local), jnp.bfloat16),
            pltpu.VMEM((param_count, stripe, gauge_local), jnp.bfloat16),
            pltpu.VMEM((2 * sample_total, LANES), jnp.float32),
            pltpu.VMEM((sample_total, 2, LANES), jnp.float32),
            pltpu.VMEM((qoi_count * param_count, 2, LANES), jnp.float32),
            dma(()),
            dma((2,)),
            dma((LOADS,)),
            dma(()),
            dma((aligned // LANES + 1,)),
            dma(()),
            dma(()),
            dma(()),
            dma(()),
            pltpu.SemaphoreType.REGULAR,
        ],
        compiler_params=pltpu.CompilerParams(
            collective_id=0, has_side_effects=True, vmem_limit_bytes=53 * 2**20
        ),
    )(
        block_start,
        pltpu.with_memory_space_constraint(gauge_group.reshape(1, gauge_local), pltpu.HBM),
        samples.transpose(2, 0, 1),
        rows,
    )
    return pl.pallas_call(
        writer,
        out_shape=shapes,
        in_specs=[vmem, vmem],
        out_specs=(pl.BlockSpec(memory_space=pl.ANY), pl.BlockSpec(memory_space=pl.ANY)),
        scratch_shapes=[dma((2,))],
    )(*[pltpu.with_memory_space_constraint(array, pltpu.VMEM) for array in found])


def solution(mesh):
    return jax.shard_map(
        local,
        mesh=mesh,
        in_specs=(P("qoi", "param", None), P(None, "param", None, "qoi"), P(), P("qoi")),
        out_specs=(P("param", None, None, "qoi"), P("param", None, None, None)),
        check_vma=False,
    )
```

```python
import functools
import math

import jax
import jax.numpy as jnp
from jax import lax
from jax.experimental import pallas as pl
from jax.experimental.pallas import tpu as pltpu
from jax.sharding import PartitionSpec as P

GROUPS = 16
LANES = 128
LOADS = 1
MESH = pl.DeviceIdType.MESH
NT_DIMS = (((1,), (1,)), ((), ()))


def pairwise(terms):
    while len(terms) > 1:
        terms = [sum(terms[i + 1 : i + 2], terms[i]) for i in range(0, len(terms), 2)]
    return terms[0]


def build_table(start, freq_count, steps_count, count, repeat, table):
    shape = (freq_count, count * repeat)
    steps = lax.broadcasted_iota(jnp.int32, shape, 1) // repeat
    freqs = lax.broadcasted_iota(jnp.int32, shape, 0) + start
    turns = (steps * freqs).astype(jnp.float32)
    whole = jnp.floor((turns + 0.5) * (1.0 / steps_count))
    phases = (turns - whole * steps_count) * (2.0 * math.pi / steps_count)
    scale = 1.0 / math.sqrt(steps_count)
    waves = [jnp.cos(phases) * scale, jnp.sin(phases) * -scale]
    highs = [wave.astype(jnp.bfloat16).astype(jnp.float32) for wave in waves]
    lows = [wave - high for wave, high in zip(waves, highs)]
    full = (repeat, count * repeat)
    keep = lax.broadcasted_iota(jnp.int32, full, 1) % repeat == lax.broadcasted_iota(
        jnp.int32, full, 0
    )
    for level, pair in enumerate((highs, lows)):
        for f in range(freq_count):
            rows = jnp.concatenate(
                [jnp.where(keep, jnp.broadcast_to(wave[f : f + 1], full), 0.0) for wave in pair],
                axis=0,
            )
            first = (level * freq_count + f) * 2 * repeat
            table[pl.ds(first, 2 * repeat), :] = rows.astype(jnp.bfloat16)


def kernel(
    param_count, qoi_count, start_ref, group_hbm, samples_hbm, rows_hbm,
    out_ref, seg_ref,
    group_ref, samples, table, weights, loose, dense, dense_tail, grouped, grouped_tail, hot, line, near, far, outgoing, incoming, joined, shares, gathered,
    group_sem, samples_sem, weights_sem, line_send, line_recv, out_send, out_recv, share_send, share_recv, known,
):
    steps_count, sample_local, param_local = samples.shape
    freq_count = weights.shape[0]
    gauge_local = group_ref.shape[1]
    halves = gauge_local // LANES
    aligned = param_local // LANES * LANES
    tail = param_local - aligned
    chunks = aligned // LANES
    pair_rows = 2 * sample_local
    half_freqs = freq_count // 2
    half_steps = steps_count // 2
    stripe = 2 * freq_count
    inner = 2 ** (int(math.log2(param_count)) // 2)
    me_p = lax.axis_index("param")
    me_q = lax.axis_index("qoi")
    base = me_p // inner * inner

    contacts = []
    for turn in range(1, param_count // inner):
        contacts.append((lax.rem(me_p + turn * inner, param_count), me_q))
    for other in reversed(range(qoi_count)):
        for turn in range(inner):
            if other or turn:
                contacts.append(
                    (base + lax.rem(me_p + turn, inner), lax.rem(me_q + other, qoi_count))
                )
    barrier = pltpu.get_barrier_semaphore()
    lanes = [pl.ds(0, aligned), pl.ds(aligned, tail)]
    sample_copies = [
        pltpu.make_async_copy(samples_hbm.at[:, :, lane], samples.at[:, :, lane], samples_sem.at[part])
        for part, lane in enumerate(lanes)
    ]
    for copy in sample_copies:
        copy.start()
    group_copy = pltpu.make_async_copy(group_hbm, group_ref, group_sem)
    group_copy.start()
    for contact in contacts:
        pl.semaphore_signal(barrier, inc=1, device_id=contact, device_id_type=MESH)
    per_load = freq_count // LOADS
    loads = [pl.ds(load * per_load, per_load) for load in range(LOADS)]
    weight_copies = [
        pltpu.make_async_copy(rows_hbm.at[load], weights.at[load], weights_sem.at[index])
        for index, load in enumerate(loads)
    ]

    start = start_ref[0]
    build_table(start, freq_count, steps_count, half_steps, sample_local, table)
    for copy in weight_copies:
        copy.start()

    sample_copies[0].wait()

    def send_line(first, count, index):
        picked = pl.ds(first, count)
        for offset in range(1, qoi_count):
            pltpu.make_async_remote_copy(
                src_ref=line.at[me_q, picked],
                dst_ref=line.at[me_q, picked],
                send_sem=line_send,
                recv_sem=line_recv.at[index],
                device_id=(me_p, lax.rem(me_q + offset, qoi_count)),
                device_id_type=MESH,
            ).start()

    def wait_line(first, count, index):
        others = line.at[pl.ds(0, qoi_count - 1), pl.ds(first, count)]
        return pltpu.make_async_remote_copy(
            src_ref=others,
            dst_ref=others,
            send_sem=line_send,
            recv_sem=line_recv.at[index],
            device_id=(me_p, lax.rem(me_q + 1, qoi_count)),
            device_id_type=MESH,
        )

    turns = table[...]
    half = freq_count * pair_rows
    sides, ends = [], []
    for part in range(2):
        block = samples[pl.ds(part * half_steps, half_steps), :, pl.ds(0, aligned)]
        block = block.reshape(half_steps * sample_local, aligned)
        both = jnp.dot(turns, block, preferred_element_type=jnp.float32)
        sides.append(both[:half] + both[half:])
    odd = lax.rem(start + lax.broadcasted_iota(jnp.int32, (half, LANES), 0) // pair_rows, 2)
    sign = 1.0 - 2.0 * odd.astype(jnp.float32)
    pl.semaphore_wait(barrier, len(contacts))
    for chunk in range(chunks):
        columns = slice(chunk * LANES, (chunk + 1) * LANES)
        spectrum = sides[0][:, columns] + sign * sides[1][:, columns]
        line[me_q, chunk * freq_count : (chunk + 1) * freq_count] = spectrum.astype(
            jnp.bfloat16
        ).reshape(freq_count, pair_rows, LANES)
        send_line(chunk * freq_count, freq_count, chunk)
    for contact in contacts:
        pl.semaphore_signal(known, inc=1, device_id=contact, device_id_type=MESH)
    sample_copies[1].wait()
    for part in range(2):
        block = samples[pl.ds(part * half_steps, half_steps), :, pl.ds(aligned, tail)]
        ends.append(block.reshape(half_steps * sample_local, tail))
    both = jnp.dot(turns, jnp.concatenate(ends, axis=1), preferred_element_type=jnp.float32)
    both = both[:half] + both[half:]
    both = both + sign * pltpu.roll(both, tail, 1)
    middle = half // 2
    lane = lax.broadcasted_iota(jnp.int32, (middle, LANES), 1)
    packed = jnp.where(lane < tail, both[:middle], both[middle:] * sign[middle:])
    line[me_q, chunks * freq_count :] = packed.astype(jnp.bfloat16).reshape(
        half_freqs, pair_rows, LANES
    )
    send_line(chunks * freq_count, half_freqs, chunks)

    group_copy.wait()
    slots = lax.broadcasted_iota(jnp.int32, (LANES, gauge_local), 0)
    for f in range(freq_count):
        place = (freq_count - f) % freq_count * GROUPS
        hot[f] = (slots == group_ref[...] + place).astype(jnp.float32).astype(jnp.bfloat16)

    for f in range(freq_count):
        if f % per_load == 0:
            weight_copies[f // per_load].wait()
        loose[...] = weights[f].astype(jnp.float32)
        for part in range(2):
            piece = jnp.concatenate(
                [
                    loose[pl.ds(2 * j + part, param_local, stride=2 * halves), :]
                    for j in range(halves)
                ],
                axis=1,
            ).astype(jnp.bfloat16)
            dense[f, part] = piece[:aligned]
            dense_tail[f % half_freqs, part, pl.ds(f // half_freqs * tail, tail)] = piece[aligned:]

    mine = me_q * param_count + me_p
    ratio = math.sqrt(GROUPS / (gauge_local * qoi_count))

    def combine(sides):
        real, imag = sides
        results = [[], []]
        for index in range(real.shape[0] // pair_rows):
            low, mid, high = [index * pair_rows + step * sample_local for step in range(3)]
            results[0].append(real[low:mid] - imag[mid:high])
            results[1].append(imag[low:mid] + real[mid:high])
        return [jnp.concatenate(result, axis=0) for result in results]

    def multiply(owners, f, chunk):
        if chunk < chunks:
            left = jnp.concatenate([line[q, chunk * freq_count + f] for q in owners], axis=0)
            right = [dense[f, part, chunk * LANES : (chunk + 1) * LANES, :] for part in range(2)]
        else:
            left = jnp.concatenate(
                [line[q, chunks * freq_count + f % half_freqs] for q in owners], axis=0
            )
            lane = lax.broadcasted_iota(jnp.int32, left.shape, 1)
            left = jnp.where((lane >= tail) == (f >= half_freqs), left.astype(jnp.float32), 0.0)
            left = left.astype(jnp.bfloat16)
            right = [dense_tail[f % half_freqs, part] for part in range(2)]
        return combine(
            [jnp.dot(left, side, preferred_element_type=jnp.float32) for side in right]
        )

    def build_grouped():
        for f in range(freq_count):
            ending = pl.ds(f // half_freqs * tail, tail)
            rows = []
            for part in range(2):
                rows += [dense[f, part], dense_tail[f % half_freqs, part, ending]]
            sums = lax.dot_general(
                jnp.concatenate(rows, axis=0), hot[f], NT_DIMS, preferred_element_type=jnp.float32
            ).astype(jnp.bfloat16)
            for part in range(2):
                first = part * param_local
                for chunk in range(chunks):
                    row = first + chunk * LANES
                    grouped[chunk, part, f] = sums[row : row + LANES]
                grouped_tail[f % half_freqs, part, ending] = sums[
                    first + aligned : first + param_local
                ]

    def group_products(owners, chunk):
        tiles = freq_count if chunk < chunks else half_freqs
        left = jnp.concatenate(
            [
                jnp.concatenate([line[q, chunk * freq_count + tile] for tile in range(tiles)], axis=1)
                for q in owners
            ],
            axis=0,
        )
        right = grouped.at[chunk] if chunk < chunks else grouped_tail
        results = []
        for part in range(2):
            if chunk < chunks:
                side = right[part]
            else:
                side = jnp.stack([right[tile, part] for tile in range(tiles)], axis=0)
            side = side.reshape(tiles * LANES, LANES)
            results.append(jnp.dot(left, side, preferred_element_type=jnp.float32))
        return results

    def rows_of(k, f, count):
        return pl.ds((k * freq_count + f) * count, count)

    def deliver_shares(owners, segment):
        count = len(owners) * sample_local
        joined[pl.ds(0, 2 * count), :] = segment * ratio
        for index, q in enumerate(owners):
            for i in range(sample_local):
                shares[q * sample_local + i] = joined[
                    pl.ds(index * sample_local + i, 2, stride=count), :
                ]
        for away in reversed(range(qoi_count)):
            for q in owners:
                for i in range(sample_local):
                    target = q * sample_local + i
                    copy = pltpu.make_async_remote_copy(
                        src_ref=shares.at[target],
                        dst_ref=gathered.at[mine],
                        send_sem=share_send,
                        recv_sem=share_recv,
                        device_id=(target, lax.rem(me_q + away, qoi_count)),
                        device_id_type=MESH,
                    )
                    if away:
                        copy.start()
                    else:
                        pl.when(target != me_p)(copy.start)

    def deliver_blocks(owners, product):
        count = len(owners) * sample_local
        for index, q in enumerate(owners):
            for i in range(sample_local):
                for j in range(halves):
                    outgoing[q * sample_local + i, :, j * LANES : (j + 1) * LANES] = product[
                        j, pl.ds(index * sample_local + i, stripe, stride=count), :
                    ].astype(jnp.bfloat16)
        for q in owners:
            for i in range(sample_local):
                target = q * sample_local + i
                copy = pltpu.make_async_remote_copy(
                    src_ref=outgoing.at[target],
                    dst_ref=incoming.at[me_p],
                    send_sem=out_send,
                    recv_sem=out_recv,
                    device_id=(target, me_q),
                    device_id_type=MESH,
                )
                pl.when(target != me_p)(copy.start)

    def add_products(owners, product, chunk):
        count = len(owners) * sample_local
        for f in range(freq_count):
            for k, value in enumerate(multiply(owners, f, chunk)):
                for j in range(halves):
                    here = value[:, j * LANES : (j + 1) * LANES]
                    if chunk:
                        here = here + product[j, rows_of(k, f, count), :]
                    product[j, rows_of(k, f, count), :] = here

    def await_known():
        pl.semaphore_wait(known, len(contacts))

    def wait_chunk(chunk):
        rows = freq_count if chunk < chunks else half_freqs
        wait_line(chunk * freq_count, rows, chunk).wait_recv()

    def send_shares(owners, before_chunk, before_sending, after_chunk):
        totals = None
        for chunk in range(chunks + 1):
            before_chunk(chunk)
            sums = group_products(owners, chunk)
            totals = sums if totals is None else [a + b for a, b in zip(totals, sums)]
            if chunk == chunks:
                before_sending()
                deliver_shares(owners, jnp.concatenate(combine(totals), axis=0))
            after_chunk(chunk)

    def nothing(*_):
        pass

    def receive(owners, product, before_sending):
        def early(chunk):
            if chunk < chunks - 1:
                add_products(owners, product, chunk)

        send_shares(owners, wait_chunk, before_sending, early)
        for chunk in range(max(chunks - 1, 0), chunks + 1):
            add_products(owners, product, chunk)
        deliver_blocks(owners, product)

    def serve(owners, product, before_sending, after_blocks):
        for chunk in range(chunks + 1):
            add_products(owners, product, chunk)
        before_sending()
        deliver_blocks(owners, product)
        after_blocks()
        send_shares(owners, nothing, nothing, nothing)

    rest = list(range(1, qoi_count))

    @pl.when(me_q == 0)
    def _():
        serve([0], near, await_known, build_grouped)
        receive(rest, far, nothing)

    @pl.when(me_q != 0)
    def _():
        build_grouped()
        receive([0], near, await_known)
        serve(rest, far, nothing, nothing)

    incoming[me_p] = outgoing[me_p]
    gathered[mine] = shares[me_p]

    aside = (lax.rem(me_p + 1, param_count), me_q)
    others = incoming.at[pl.ds(0, param_count - 1)]
    out_wait = pltpu.make_async_remote_copy(
        src_ref=others, dst_ref=others, send_sem=out_send, recv_sem=out_recv,
        device_id=aside, device_id_type=MESH,
    )
    others = gathered.at[pl.ds(0, qoi_count * param_count - 1)]
    share_wait = pltpu.make_async_remote_copy(
        src_ref=others, dst_ref=others, send_sem=share_send, recv_sem=share_recv,
        device_id=aside, device_id_type=MESH,
    )
    out_wait.wait_recv()
    total = pairwise([incoming[p].astype(jnp.float32) for p in range(param_count)])
    out_ref[...] = total.reshape(out_ref.shape)
    wait_line(0, chunks * freq_count + half_freqs, 0).wait_send()
    out_wait.wait_send()
    share_wait.wait_send()
    share_wait.wait_recv()
    final = pairwise([gathered[p] for p in range(param_count * qoi_count)])
    for k in range(2):
        rows = jnp.broadcast_to(final[k : k + 1], (freq_count, LANES))
        turned = pltpu.roll(rows, 0, 1, stride=GROUPS, stride_axis=0)
        seg_ref[0, k] = turned[:, :GROUPS]


def writer(spectrum_ref, response_ref, spectrum_hbm, response_hbm, sems):
    copies = [
        pltpu.make_async_copy(spectrum_ref, spectrum_hbm, sems.at[0]),
        pltpu.make_async_copy(response_ref, response_hbm, sems.at[1]),
    ]
    for copy in copies:
        copy.start()
    for copy in copies:
        copy.wait()


def local(samples, operator_rows, block_start, gauge_group):
    sample_local, param_local, steps_count = samples.shape
    freq_count, _, _, gauge_local = operator_rows.shape
    param_count, qoi_count = lax.axis_size("param"), lax.axis_size("qoi")
    sample_total = sample_local * qoi_count
    halves = gauge_local // LANES
    depth = 2 * param_local
    stripe = 2 * freq_count
    aligned = param_local // LANES * LANES
    tail = param_local - aligned
    assert sample_total == param_count and freq_count * GROUPS == LANES
    assert 2 * tail == LANES and freq_count % LOADS == 0 and steps_count % 2 == 0
    rows = operator_rows.reshape(freq_count, param_local, 2, halves, LANES)
    rows = rows.transpose(0, 1, 3, 2, 4).reshape(freq_count, depth * halves, LANES)
    dma = pltpu.SemaphoreType.DMA
    vmem = pl.BlockSpec(memory_space=pltpu.VMEM)
    hbm = pl.BlockSpec(memory_space=pltpu.HBM)
    shapes = (
        jax.ShapeDtypeStruct((1, 2, freq_count, gauge_local), jnp.float32),
        jax.ShapeDtypeStruct((1, 2, freq_count, GROUPS), jnp.float32),
    )
    found = pl.pallas_call(
        functools.partial(kernel, param_count, qoi_count),
        out_shape=shapes,
        in_specs=[pl.BlockSpec(memory_space=pltpu.SMEM), hbm, hbm, hbm],
        out_specs=(vmem, vmem),
        scratch_shapes=[
            pltpu.VMEM((1, gauge_local), jnp.int32),
            pltpu.VMEM((steps_count, sample_local, param_local), jnp.bfloat16),
            pltpu.VMEM((4 * freq_count * sample_local, steps_count // 2 * sample_local), jnp.bfloat16),
            pltpu.VMEM((freq_count, depth * halves, LANES), jnp.bfloat16),
            pltpu.VMEM((depth * halves, LANES), jnp.float32),
            pltpu.VMEM((freq_count, 2, aligned, gauge_local), jnp.bfloat16),
            pltpu.VMEM((freq_count // 2, 2, 2 * tail, gauge_local), jnp.bfloat16),
            pltpu.VMEM((aligned // LANES, 2, freq_count, LANES, LANES), jnp.bfloat16),
            pltpu.VMEM((freq_count // 2, 2, 2 * tail, LANES), jnp.bfloat16),
            pltpu.VMEM((freq_count, LANES, gauge_local), jnp.bfloat16),
            pltpu.VMEM(
                (qoi_count, aligned // LANES * freq_count + freq_count // 2, 2 * sample_local, LANES),
                jnp.bfloat16,
            ),
            pltpu.VMEM((halves, stripe * sample_local, LANES), jnp.float32),
            pltpu.VMEM((halves, stripe * (sample_total - sample_local), LANES), jnp.float32),
            pltpu.VMEM((sample_total, stripe, gauge_local), jnp.bfloat16),
            pltpu.VMEM((param_count, stripe, gauge_local), jnp.bfloat16),
            pltpu.VMEM((2 * sample_total, LANES), jnp.float32),
            pltpu.VMEM((sample_total, 2, LANES), jnp.float32),
            pltpu.VMEM((qoi_count * param_count, 2, LANES), jnp.float32),
            dma(()),
            dma((2,)),
            dma((LOADS,)),
            dma(()),
            dma((aligned // LANES + 1,)),
            dma(()),
            dma(()),
            dma(()),
            dma(()),
            pltpu.SemaphoreType.REGULAR,
        ],
        compiler_params=pltpu.CompilerParams(
            collective_id=0, has_side_effects=True, vmem_limit_bytes=53 * 2**20
        ),
    )(
        block_start,
        pltpu.with_memory_space_constraint(gauge_group.reshape(1, gauge_local), pltpu.HBM),
        samples.transpose(2, 0, 1),
        rows,
    )
    return pl.pallas_call(
        writer,
        out_shape=shapes,
        in_specs=[vmem, vmem],
        out_specs=(pl.BlockSpec(memory_space=pl.ANY), pl.BlockSpec(memory_space=pl.ANY)),
        scratch_shapes=[dma((2,))],
    )(*[pltpu.with_memory_space_constraint(array, pltpu.VMEM) for array in found])


def solution(mesh):
    return jax.shard_map(
        local,
        mesh=mesh,
        in_specs=(P("qoi", "param", None), P(None, "param", None, "qoi"), P(), P("qoi")),
        out_specs=(P("param", None, None, "qoi"), P("param", None, None, None)),
        check_vma=False,
    )
```

```python
import functools
import math

import jax
import jax.numpy as jnp
from jax import lax
from jax.experimental import pallas as pl
from jax.experimental.pallas import tpu as pltpu
from jax.sharding import PartitionSpec as P

GROUPS = 16
LANES = 128
LOADS = 1
MESH = pl.DeviceIdType.MESH
NT_DIMS = (((1,), (1,)), ((), ()))


def pairwise(terms):
    while len(terms) > 1:
        terms = [sum(terms[i + 1 : i + 2], terms[i]) for i in range(0, len(terms), 2)]
    return terms[0]


def build_table(start, freq_count, steps_count, count, repeat, table):
    shape = (freq_count, count * repeat)
    steps = lax.broadcasted_iota(jnp.int32, shape, 1) // repeat
    freqs = lax.broadcasted_iota(jnp.int32, shape, 0) + start
    turns = (steps * freqs).astype(jnp.float32)
    whole = jnp.floor((turns + 0.5) * (1.0 / steps_count))
    phases = (turns - whole * steps_count) * (2.0 * math.pi / steps_count)
    scale = 1.0 / math.sqrt(steps_count)
    waves = [jnp.cos(phases) * scale, jnp.sin(phases) * -scale]
    highs = [wave.astype(jnp.bfloat16).astype(jnp.float32) for wave in waves]
    lows = [wave - high for wave, high in zip(waves, highs)]
    full = (repeat, count * repeat)
    keep = lax.broadcasted_iota(jnp.int32, full, 1) % repeat == lax.broadcasted_iota(
        jnp.int32, full, 0
    )
    for level, pair in enumerate((highs, lows)):
        for f in range(freq_count):
            rows = jnp.concatenate(
                [jnp.where(keep, jnp.broadcast_to(wave[f : f + 1], full), 0.0) for wave in pair],
                axis=0,
            )
            first = (level * freq_count + f) * 2 * repeat
            table[pl.ds(first, 2 * repeat), :] = rows.astype(jnp.bfloat16)


def kernel(
    param_count, qoi_count, start_ref, group_hbm, samples_hbm, rows_hbm,
    out_ref, seg_ref,
    group_ref, samples, table, weights, loose, dense, dense_tail, grouped, grouped_tail, hot, line, near, far, outgoing, incoming, joined, shares, gathered,
    group_sem, samples_sem, weights_sem, line_send, line_recv, out_send, out_recv, share_send, share_recv, known,
):
    steps_count, sample_local, param_local = samples.shape
    freq_count = weights.shape[0]
    gauge_local = group_ref.shape[1]
    halves = gauge_local // LANES
    aligned = param_local // LANES * LANES
    tail = param_local - aligned
    chunks = aligned // LANES
    pair_rows = 2 * sample_local
    half_freqs = freq_count // 2
    half_steps = steps_count // 2
    stripe = 2 * freq_count
    inner = 2 ** (int(math.log2(param_count)) // 2)
    me_p = lax.axis_index("param")
    me_q = lax.axis_index("qoi")
    base = me_p // inner * inner

    contacts = []
    for turn in range(1, param_count // inner):
        contacts.append((lax.rem(me_p + turn * inner, param_count), me_q))
    for other in reversed(range(qoi_count)):
        for turn in range(inner):
            if other or turn:
                contacts.append(
                    (base + lax.rem(me_p + turn, inner), lax.rem(me_q + other, qoi_count))
                )
    barrier = pltpu.get_barrier_semaphore()
    lanes = [pl.ds(0, aligned), pl.ds(aligned, tail)]
    sample_copies = [
        pltpu.make_async_copy(samples_hbm.at[:, :, lane], samples.at[:, :, lane], samples_sem.at[part])
        for part, lane in enumerate(lanes)
    ]
    for copy in sample_copies:
        copy.start()
    group_copy = pltpu.make_async_copy(group_hbm, group_ref, group_sem)
    group_copy.start()
    for contact in contacts:
        pl.semaphore_signal(barrier, inc=1, device_id=contact, device_id_type=MESH)
    per_load = freq_count // LOADS
    loads = [pl.ds(load * per_load, per_load) for load in range(LOADS)]
    weight_copies = [
        pltpu.make_async_copy(rows_hbm.at[load], weights.at[load], weights_sem.at[index])
        for index, load in enumerate(loads)
    ]

    start = start_ref[0]
    build_table(start, freq_count, steps_count, half_steps, sample_local, table)
    for copy in weight_copies:
        copy.start()

    sample_copies[0].wait()

    def send_line(first, count, index):
        picked = pl.ds(first, count)
        for offset in range(1, qoi_count):
            pltpu.make_async_remote_copy(
                src_ref=line.at[me_q, picked],
                dst_ref=line.at[me_q, picked],
                send_sem=line_send,
                recv_sem=line_recv.at[index],
                device_id=(me_p, lax.rem(me_q + offset, qoi_count)),
                device_id_type=MESH,
            ).start()

    def wait_line(first, count, index):
        others = line.at[pl.ds(0, qoi_count - 1), pl.ds(first, count)]
        return pltpu.make_async_remote_copy(
            src_ref=others,
            dst_ref=others,
            send_sem=line_send,
            recv_sem=line_recv.at[index],
            device_id=(me_p, lax.rem(me_q + 1, qoi_count)),
            device_id_type=MESH,
        )

    turns = table[...]
    half = freq_count * pair_rows
    sides, ends = [], []
    for part in range(2):
        block = samples[pl.ds(part * half_steps, half_steps), :, pl.ds(0, aligned)]
        block = block.reshape(half_steps * sample_local, aligned)
        both = jnp.dot(turns, block, preferred_element_type=jnp.float32)
        sides.append(both[:half] + both[half:])
    odd = lax.rem(start + lax.broadcasted_iota(jnp.int32, (half, LANES), 0) // pair_rows, 2)
    sign = 1.0 - 2.0 * odd.astype(jnp.float32)
    pl.semaphore_wait(barrier, len(contacts))
    for chunk in range(chunks):
        columns = slice(chunk * LANES, (chunk + 1) * LANES)
        spectrum = sides[0][:, columns] + sign * sides[1][:, columns]
        line[me_q, chunk * freq_count : (chunk + 1) * freq_count] = spectrum.astype(
            jnp.bfloat16
        ).reshape(freq_count, pair_rows, LANES)
        send_line(chunk * freq_count, freq_count, chunk)
    for contact in contacts:
        pl.semaphore_signal(known, inc=1, device_id=contact, device_id_type=MESH)
    sample_copies[1].wait()
    for part in range(2):
        block = samples[pl.ds(part * half_steps, half_steps), :, pl.ds(aligned, tail)]
        ends.append(block.reshape(half_steps * sample_local, tail))
    both = jnp.dot(turns, jnp.concatenate(ends, axis=1), preferred_element_type=jnp.float32)
    both = both[:half] + both[half:]
    both = both + sign * pltpu.roll(both, tail, 1)
    middle = half // 2
    lane = lax.broadcasted_iota(jnp.int32, (middle, LANES), 1)
    packed = jnp.where(lane < tail, both[:middle], both[middle:] * sign[middle:])
    line[me_q, chunks * freq_count :] = packed.astype(jnp.bfloat16).reshape(
        half_freqs, pair_rows, LANES
    )
    send_line(chunks * freq_count, half_freqs, chunks)

    group_copy.wait()
    slots = lax.broadcasted_iota(jnp.int32, (LANES, gauge_local), 0)
    for f in range(freq_count):
        place = (freq_count - f) % freq_count * GROUPS
        hot[f] = (slots == group_ref[...] + place).astype(jnp.float32).astype(jnp.bfloat16)

    for f in range(freq_count):
        if f % per_load == 0:
            weight_copies[f // per_load].wait()
        loose[...] = weights[f].astype(jnp.float32)
        for part in range(2):
            piece = jnp.concatenate(
                [
                    loose[pl.ds(2 * j + part, param_local, stride=2 * halves), :]
                    for j in range(halves)
                ],
                axis=1,
            ).astype(jnp.bfloat16)
            dense[f, part] = piece[:aligned]
            dense_tail[f % half_freqs, part, pl.ds(f // half_freqs * tail, tail)] = piece[aligned:]

    mine = me_q * param_count + me_p
    ratio = math.sqrt(GROUPS / (gauge_local * qoi_count))

    def combine(sides):
        real, imag = sides
        results = [[], []]
        for index in range(real.shape[0] // pair_rows):
            low, mid, high = [index * pair_rows + step * sample_local for step in range(3)]
            results[0].append(real[low:mid] - imag[mid:high])
            results[1].append(imag[low:mid] + real[mid:high])
        return [jnp.concatenate(result, axis=0) for result in results]

    def multiply(owners, f, chunk):
        if chunk < chunks:
            left = jnp.concatenate([line[q, chunk * freq_count + f] for q in owners], axis=0)
            right = [dense[f, part, chunk * LANES : (chunk + 1) * LANES, :] for part in range(2)]
        else:
            left = jnp.concatenate(
                [line[q, chunks * freq_count + f % half_freqs] for q in owners], axis=0
            )
            lane = lax.broadcasted_iota(jnp.int32, left.shape, 1)
            left = jnp.where((lane >= tail) == (f >= half_freqs), left.astype(jnp.float32), 0.0)
            left = left.astype(jnp.bfloat16)
            right = [dense_tail[f % half_freqs, part] for part in range(2)]
        return combine(
            [jnp.dot(left, side, preferred_element_type=jnp.float32) for side in right]
        )

    def build_grouped():
        for f in range(freq_count):
            ending = pl.ds(f // half_freqs * tail, tail)
            rows = []
            for part in range(2):
                rows += [dense[f, part], dense_tail[f % half_freqs, part, ending]]
            sums = lax.dot_general(
                jnp.concatenate(rows, axis=0), hot[f], NT_DIMS, preferred_element_type=jnp.float32
            ).astype(jnp.bfloat16)
            for part in range(2):
                first = part * param_local
                for chunk in range(chunks):
                    row = first + chunk * LANES
                    grouped[chunk, part, f] = sums[row : row + LANES]
                grouped_tail[f % half_freqs, part, ending] = sums[
                    first + aligned : first + param_local
                ]

    def group_products(owners, chunk):
        tiles = freq_count if chunk < chunks else half_freqs
        left = jnp.concatenate(
            [
                jnp.concatenate([line[q, chunk * freq_count + tile] for tile in range(tiles)], axis=1)
                for q in owners
            ],
            axis=0,
        )
        right = grouped.at[chunk] if chunk < chunks else grouped_tail
        results = []
        for part in range(2):
            if chunk < chunks:
                side = right[part]
            else:
                side = jnp.stack([right[tile, part] for tile in range(tiles)], axis=0)
            side = side.reshape(tiles * LANES, LANES)
            results.append(jnp.dot(left, side, preferred_element_type=jnp.float32))
        return results

    def rows_of(k, f, count):
        return pl.ds((k * freq_count + f) * count, count)

    def deliver_shares(owners, segment):
        count = len(owners) * sample_local
        joined[pl.ds(0, 2 * count), :] = segment * ratio
        for index, q in enumerate(owners):
            for i in range(sample_local):
                shares[q * sample_local + i] = joined[
                    pl.ds(index * sample_local + i, 2, stride=count), :
                ]
        for away in reversed(range(qoi_count)):
            for q in owners:
                for i in range(sample_local):
                    target = q * sample_local + i
                    copy = pltpu.make_async_remote_copy(
                        src_ref=shares.at[target],
                        dst_ref=gathered.at[mine],
                        send_sem=share_send,
                        recv_sem=share_recv,
                        device_id=(target, lax.rem(me_q + away, qoi_count)),
                        device_id_type=MESH,
                    )
                    if away:
                        copy.start()
                    else:
                        pl.when(target != me_p)(copy.start)

    def deliver_blocks(owners, product):
        count = len(owners) * sample_local
        for index, q in enumerate(owners):
            for i in range(sample_local):
                for j in range(halves):
                    outgoing[q * sample_local + i, :, j * LANES : (j + 1) * LANES] = product[
                        j, pl.ds(index * sample_local + i, stripe, stride=count), :
                    ].astype(jnp.bfloat16)
        for q in owners:
            for i in range(sample_local):
                target = q * sample_local + i
                copy = pltpu.make_async_remote_copy(
                    src_ref=outgoing.at[target],
                    dst_ref=incoming.at[me_p],
                    send_sem=out_send,
                    recv_sem=out_recv,
                    device_id=(target, me_q),
                    device_id_type=MESH,
                )
                pl.when(target != me_p)(copy.start)

    def add_products(owners, product, chunk):
        count = len(owners) * sample_local
        for f in range(freq_count):
            for k, value in enumerate(multiply(owners, f, chunk)):
                for j in range(halves):
                    here = value[:, j * LANES : (j + 1) * LANES]
                    if chunk:
                        here = here + product[j, rows_of(k, f, count), :]
                    product[j, rows_of(k, f, count), :] = here

    def await_known():
        pl.semaphore_wait(known, len(contacts))

    def wait_chunk(chunk):
        rows = freq_count if chunk < chunks else half_freqs
        wait_line(chunk * freq_count, rows, chunk).wait_recv()

    def send_shares(owners, before_chunk, before_sending, after_chunk):
        totals = None
        for chunk in range(chunks + 1):
            if chunk == chunks:
                before_sending()
            before_chunk(chunk)
            sums = group_products(owners, chunk)
            totals = sums if totals is None else [a + b for a, b in zip(totals, sums)]
            if chunk == chunks:
                deliver_shares(owners, jnp.concatenate(combine(totals), axis=0))
            after_chunk(chunk)

    def nothing(*_):
        pass

    def receive(owners, product, before_sending):
        def early(chunk):
            if chunk < chunks - 1:
                add_products(owners, product, chunk)

        send_shares(owners, wait_chunk, before_sending, early)
        for chunk in range(max(chunks - 1, 0), chunks + 1):
            add_products(owners, product, chunk)
        deliver_blocks(owners, product)

    def serve(owners, product, before_sending, after_blocks):
        for chunk in range(chunks + 1):
            add_products(owners, product, chunk)
        before_sending()
        deliver_blocks(owners, product)
        after_blocks()
        send_shares(owners, nothing, nothing, nothing)

    rest = list(range(1, qoi_count))

    @pl.when(me_q == 0)
    def _():
        serve([0], near, await_known, build_grouped)
        receive(rest, far, nothing)

    @pl.when(me_q != 0)
    def _():
        build_grouped()
        receive([0], near, await_known)
        serve(rest, far, nothing, nothing)

    incoming[me_p] = outgoing[me_p]
    gathered[mine] = shares[me_p]

    aside = (lax.rem(me_p + 1, param_count), me_q)
    others = incoming.at[pl.ds(0, param_count - 1)]
    out_wait = pltpu.make_async_remote_copy(
        src_ref=others, dst_ref=others, send_sem=out_send, recv_sem=out_recv,
        device_id=aside, device_id_type=MESH,
    )
    others = gathered.at[pl.ds(0, qoi_count * param_count - 1)]
    share_wait = pltpu.make_async_remote_copy(
        src_ref=others, dst_ref=others, send_sem=share_send, recv_sem=share_recv,
        device_id=aside, device_id_type=MESH,
    )
    out_wait.wait_recv()
    total = pairwise([incoming[p].astype(jnp.float32) for p in range(param_count)])
    out_ref[...] = total.reshape(out_ref.shape)
    wait_line(0, chunks * freq_count + half_freqs, 0).wait_send()
    out_wait.wait_send()
    share_wait.wait_send()
    share_wait.wait_recv()
    final = pairwise([gathered[p] for p in range(param_count * qoi_count)])
    for k in range(2):
        rows = jnp.broadcast_to(final[k : k + 1], (freq_count, LANES))
        turned = pltpu.roll(rows, 0, 1, stride=GROUPS, stride_axis=0)
        seg_ref[0, k] = turned[:, :GROUPS]


def writer(spectrum_ref, response_ref, spectrum_hbm, response_hbm, sems):
    copies = [
        pltpu.make_async_copy(spectrum_ref, spectrum_hbm, sems.at[0]),
        pltpu.make_async_copy(response_ref, response_hbm, sems.at[1]),
    ]
    for copy in copies:
        copy.start()
    for copy in copies:
        copy.wait()


def local(samples, operator_rows, block_start, gauge_group):
    sample_local, param_local, steps_count = samples.shape
    freq_count, _, _, gauge_local = operator_rows.shape
    param_count, qoi_count = lax.axis_size("param"), lax.axis_size("qoi")
    sample_total = sample_local * qoi_count
    halves = gauge_local // LANES
    depth = 2 * param_local
    stripe = 2 * freq_count
    aligned = param_local // LANES * LANES
    tail = param_local - aligned
    assert sample_total == param_count and freq_count * GROUPS == LANES
    assert 2 * tail == LANES and freq_count % LOADS == 0 and steps_count % 2 == 0
    rows = operator_rows.reshape(freq_count, param_local, 2, halves, LANES)
    rows = rows.transpose(0, 1, 3, 2, 4).reshape(freq_count, depth * halves, LANES)
    dma = pltpu.SemaphoreType.DMA
    vmem = pl.BlockSpec(memory_space=pltpu.VMEM)
    hbm = pl.BlockSpec(memory_space=pltpu.HBM)
    shapes = (
        jax.ShapeDtypeStruct((1, 2, freq_count, gauge_local), jnp.float32),
        jax.ShapeDtypeStruct((1, 2, freq_count, GROUPS), jnp.float32),
    )
    found = pl.pallas_call(
        functools.partial(kernel, param_count, qoi_count),
        out_shape=shapes,
        in_specs=[pl.BlockSpec(memory_space=pltpu.SMEM), hbm, hbm, hbm],
        out_specs=(vmem, vmem),
        scratch_shapes=[
            pltpu.VMEM((1, gauge_local), jnp.int32),
            pltpu.VMEM((steps_count, sample_local, param_local), jnp.bfloat16),
            pltpu.VMEM((4 * freq_count * sample_local, steps_count // 2 * sample_local), jnp.bfloat16),
            pltpu.VMEM((freq_count, depth * halves, LANES), jnp.bfloat16),
            pltpu.VMEM((depth * halves, LANES), jnp.float32),
            pltpu.VMEM((freq_count, 2, aligned, gauge_local), jnp.bfloat16),
            pltpu.VMEM((freq_count // 2, 2, 2 * tail, gauge_local), jnp.bfloat16),
            pltpu.VMEM((aligned // LANES, 2, freq_count, LANES, LANES), jnp.bfloat16),
            pltpu.VMEM((freq_count // 2, 2, 2 * tail, LANES), jnp.bfloat16),
            pltpu.VMEM((freq_count, LANES, gauge_local), jnp.bfloat16),
            pltpu.VMEM(
                (qoi_count, aligned // LANES * freq_count + freq_count // 2, 2 * sample_local, LANES),
                jnp.bfloat16,
            ),
            pltpu.VMEM((halves, stripe * sample_local, LANES), jnp.float32),
            pltpu.VMEM((halves, stripe * (sample_total - sample_local), LANES), jnp.float32),
            pltpu.VMEM((sample_total, stripe, gauge_local), jnp.bfloat16),
            pltpu.VMEM((param_count, stripe, gauge_local), jnp.bfloat16),
            pltpu.VMEM((2 * sample_total, LANES), jnp.float32),
            pltpu.VMEM((sample_total, 2, LANES), jnp.float32),
            pltpu.VMEM((qoi_count * param_count, 2, LANES), jnp.float32),
            dma(()),
            dma((2,)),
            dma((LOADS,)),
            dma(()),
            dma((aligned // LANES + 1,)),
            dma(()),
            dma(()),
            dma(()),
            dma(()),
            pltpu.SemaphoreType.REGULAR,
        ],
        compiler_params=pltpu.CompilerParams(
            collective_id=0, has_side_effects=True, vmem_limit_bytes=53 * 2**20
        ),
    )(
        block_start,
        pltpu.with_memory_space_constraint(gauge_group.reshape(1, gauge_local), pltpu.HBM),
        samples.transpose(2, 0, 1),
        rows,
    )
    return pl.pallas_call(
        writer,
        out_shape=shapes,
        in_specs=[vmem, vmem],
        out_specs=(pl.BlockSpec(memory_space=pl.ANY), pl.BlockSpec(memory_space=pl.ANY)),
        scratch_shapes=[dma((2,))],
    )(*[pltpu.with_memory_space_constraint(array, pltpu.VMEM) for array in found])


def solution(mesh):
    return jax.shard_map(
        local,
        mesh=mesh,
        in_specs=(P("qoi", "param", None), P(None, "param", None, "qoi"), P(), P("qoi")),
        out_specs=(P("param", None, None, "qoi"), P("param", None, None, None)),
        check_vma=False,
    )
```
